256 devices in a mesh: group: 2 (over y), pages: 16 (over z), heads: 8 (over x, core).
Axes of the slice: x: 4, y: 2, z: 16, core: 2. Of those that a mesh axis runs over, the one named last changes fastest.
The devices are a block of a 4x16x16 slice.
Arguments:
- queries: bfloat16 [32, 48, 128], P('group', 'heads'), parts along dimension 0, may hold values from -180 to 180
- k_cache: bfloat16 [8, 32768, 16, 128], P('heads', ('group', 'pages')), parts along dimension 1, may hold values from -6 to 6
- v_cache: bfloat16 [8, 32768, 16, 128], P('heads', ('group', 'pages')), parts along dimension 1, may hold values from -6 to 6
- new_key: bfloat16 [8, 32, 128], P('heads', 'group'), parts along dimension 1, may hold values from -6 to 6
- new_value: bfloat16 [8, 32, 128], P('heads', 'group'), parts along dimension 1, may hold values from -6 to 6
- ctx_lens: int32 [32], P('group'), parts along dimension 0, may hold values from 4081 to 16384, as said below
- page_owner: int32 [32, 1024], P('group'), parts along dimension 0, may hold values from -1 to 15, as said below
- page_slot: int32 [32, 1024], P('group'), parts along dimension 0, may hold values from 0 to 1023, as said below
- out_weight: bfloat16 [6144, 6144], P(None, 'pages'), may hold values from -0.078125 to 0.078125
Outputs:
- projected: bfloat16 [32, 6144], P(('group', 'heads'), 'pages'), parts along dimension 0
The draws below stay inside these ranges and needn't reach their ends.
There are 2 independent parts, one for each index of `group`. The reference program is written for one: setup_inputs(seed, part) draws one part's arguments, and reference() takes and returns one part's arrays. A program takes and returns all parts, laid end to end along the dimension named above; an argument that names none is the same for every part. Nothing has to cross between parts.
Inputs may be any that keep to these rules, and one draw needn't show every extreme that they name: Request r holds ceil(ctx_lens[r] / 16) pages; some request holds 16384 tokens. `page_owner`: for j below request r's page count, the device along pages that holds its logical page j; -1 beyond. No two live pages share a device and a slot. `page_slot`: for j below request r's page count, the slot of logical page j on its device; 0 beyond.
All inputs are finite; a program needn't handle non-finite values.
Results may differ from the reference program's by a relative error of at most 0.0053.
Values may be sent and summed in bfloat16 or wider, within the bound.
No kernel may reach another device: no remote copies, remote signals or barrier semaphores. Data moves between devices by JAX's collectives and lax.ppermute only.
A program may use at most 64 MiB of HBM per device.

```python
import math
import jax
import jax.numpy as jnp
from jax import lax

QH = 48
KVH = 8
HD = 128
DM = 6144
PAGE = 16
MAXP = 1024
REQS = 16
PAGES_DEV = 1024
SLOTS_ALL = 16384
N_PAGES = 16


def page_tables(key):
    base_key = jax.random.fold_in(key, 7001)
    count_key, longest_key, tail_key, shuffle_key = jax.random.split(base_key, 4)
    request_ids = jnp.arange(REQS, dtype=jnp.int32)
    fewest = max(MAXP // 4, 1)
    counts = jax.random.randint(count_key, (REQS,), fewest, MAXP + 1, dtype=jnp.int32)
    longest = jax.random.randint(longest_key, (), 0, REQS, dtype=jnp.int32)
    counts = jnp.where(request_ids == longest, MAXP, counts)
    last_rows = jax.random.randint(tail_key, (REQS,), 1, PAGE + 1, dtype=jnp.int32)
    last_rows = jnp.where(request_ids == longest, PAGE, last_rows)
    lengths = (counts - 1) * PAGE + last_rows
    shuffled = jax.random.permutation(shuffle_key, SLOTS_ALL).astype(jnp.int32)
    starts = jnp.cumsum(counts) - counts
    page_number = jnp.arange(MAXP, dtype=jnp.int32)
    flat_index = jnp.clip(starts[:, None] + page_number[None, :], 0, SLOTS_ALL - 1)
    in_use = page_number[None, :] < counts[:, None]
    chosen = shuffled[flat_index]
    page_dev = jnp.where(in_use, chosen // PAGES_DEV, -1).astype(jnp.int32)
    page_local = jnp.where(in_use, chosen % PAGES_DEV, 0).astype(jnp.int32)
    return (lengths.astype(jnp.int32), page_dev, page_local)


def query_base(key):
    drawn = jax.random.normal(jax.random.fold_in(key, 7002), (REQS, QH, HD), jnp.float32)
    return jnp.clip(drawn, -6.0, 6.0)


def draw_queries(key, part):
    base_rows = query_base(key)
    return base_rows.astype(jnp.bfloat16)


def draw_k_cache(key, part):
    drawn = jax.random.normal(jax.random.fold_in(key, 7005), (KVH, SLOTS_ALL, PAGE, HD), jnp.float32)
    drawn_cache = jnp.clip(drawn, -6.0, 6.0)
    return drawn_cache.astype(jnp.bfloat16)


def draw_ctx_lens(key, part):
    return page_tables(key)[0]


def draw_page_owner(key, part):
    return page_tables(key)[1]


def draw_page_slot(key, part):
    return page_tables(key)[2]


def levels(own_key, shape, shards, least, largest):
    level, own = 1.0, jax.random.fold_in(own_key, 6)
    for position, blocks in shards:
        steps = jnp.exp(jax.random.uniform(jax.random.fold_in(own, position), (blocks,), jnp.float32, least / len(shards), largest / len(shards)))
        level = level * jnp.repeat(steps, shape[position] // blocks).reshape([-1 if axis == position else 1 for axis in range(len(shape))])
    return level


def noise(key, shape, spread, most, pieces=(), kind=jnp.bfloat16):
    gain = levels(key, shape, pieces, -0.22, 0.18) if pieces else 1.0
    values = jax.random.normal(key, shape, jnp.float32) * spread * gain
    return jnp.minimum(jnp.maximum(values, -most), most).astype(kind)


def setup_inputs(seed: int = 0, part: int = 0) -> dict:
    arg_keys = jax.random.split(jax.random.key(seed), 10)
    own_keys = jax.random.split(jax.random.fold_in(arg_keys[9], part), 10)
    queries = draw_queries(jax.random.fold_in(jax.random.fold_in(arg_keys[9], part), 71), part)
    k_cache = draw_k_cache(jax.random.fold_in(jax.random.fold_in(arg_keys[9], part), 71), part)
    v_cache = noise(own_keys[2], (KVH, SLOTS_ALL, PAGE, HD), 1.0, 6.0, ((0, 8), (1, 16)))
    new_key = noise(own_keys[3], (KVH, REQS, HD), 1.0, 6.0, ((0, 8),))
    new_value = noise(own_keys[4], (KVH, REQS, HD), 1.0, 6.0, ((0, 8),))
    ctx_lens = draw_ctx_lens(jax.random.fold_in(jax.random.fold_in(arg_keys[9], part), 71), part)
    page_owner = draw_page_owner(jax.random.fold_in(jax.random.fold_in(arg_keys[9], part), 71), part)
    page_slot = draw_page_slot(jax.random.fold_in(jax.random.fold_in(arg_keys[9], part), 71), part)
    out_weight = noise(arg_keys[8], (QH * HD, DM), (QH * HD) ** -0.5, 0.078125, ((1, 16),))
    return {"queries": queries, "k_cache": k_cache, "v_cache": v_cache, "new_key": new_key, "new_value": new_value, "ctx_lens": ctx_lens, "page_owner": page_owner, "page_slot": page_slot, "out_weight": out_weight}


very_low = -1e+30
highest = lax.Precision.HIGHEST

def reference(queries, k_cache, v_cache, new_key, new_value, ctx_lens, page_owner, page_slot, out_weight):
    group_size = QH // KVH
    scaling = 1.0 / math.sqrt(HD)
    row_index = jnp.arange(PAGE, dtype=jnp.int32)
    page_index = jnp.arange(MAXP, dtype=jnp.int32)

    def per_request(operands):
        query, length, page_dev, page_local, key_new, value_new = operands
        global_slot = (jnp.clip(page_dev, 0, N_PAGES - 1) * PAGES_DEV + page_local).astype(jnp.int32)
        gathered_keys = k_cache[:, global_slot].astype(jnp.float32)
        gathered_values = v_cache[:, global_slot].astype(jnp.float32)
        grouped = query.reshape(KVH, group_size, HD).astype(jnp.float32)
        scores = jnp.einsum('kgd,kptd->kgpt', grouped, gathered_keys, precision=highest) * scaling
        live_rows = page_index[:, None] * PAGE + row_index[None, :] < length
        scores = jnp.where(live_rows, scores, very_low)
        page_top = lax.optimization_barrier(jnp.max(scores, axis=3))
        weights = jnp.where(live_rows, jnp.exp(scores - page_top[..., None]), 0.0)
        page_total = lax.optimization_barrier(jnp.sum(weights, axis=3))
        rounded = lax.optimization_barrier(weights.astype(jnp.bfloat16)).astype(jnp.float32)
        page_out = jnp.einsum('kgpt,kptd->kgpd', rounded, gathered_values, precision=highest)
        peak_score = lax.optimization_barrier(jnp.max(page_top, axis=2))
        factor = jnp.exp(page_top - peak_score[..., None])
        partial_out = lax.optimization_barrier(jnp.sum(page_out * factor[..., None], axis=2))
        weight_sum = lax.optimization_barrier(jnp.sum(page_total * factor, axis=2))
        self_score = jnp.einsum('kgd,kd->kg', grouped, key_new.astype(jnp.float32), precision=highest) * scaling
        peak_value = jnp.maximum(peak_score, self_score)
        keep_old = jnp.exp(peak_score - peak_value)
        take_new = jnp.exp(self_score - peak_value)
        attended = (partial_out * keep_old[..., None] + value_new.astype(jnp.float32)[:, None, :] * take_new[..., None]) / (weight_sum * keep_old + take_new)[..., None]
        return attended.reshape(QH * HD).astype(jnp.bfloat16)
    attended = lax.map(per_request, (queries, ctx_lens, page_owner, page_slot, jnp.transpose(new_key, (1, 0, 2)), jnp.transpose(new_value, (1, 0, 2))))
    return jnp.dot(attended, out_weight, preferred_element_type=jnp.float32).astype(jnp.bfloat16)
```

```python
import math

import jax
import jax.numpy as jnp
from jax import lax
from jax.experimental import pallas as pl
from jax.experimental.pallas import tpu as pltpu
from jax.sharding import Mesh
from jax.sharding import PartitionSpec as P

NEAR = 4
CHUNK = 2048
SIDE = 32
BLOCK = 8
W_CHUNKS = 6

f32 = jnp.float32
bf16 = jnp.bfloat16
masked = -1e30
lowest = -1e29


def iota(shape, dim):
    return lax.broadcasted_iota(jnp.int32, shape, dim)


def dot(a, b):
    return jnp.dot(a, b, preferred_element_type=f32)


def dot_t(a, b):
    return lax.dot_general(a, b, (((1,), (1,)), ((), ())), preferred_element_type=f32)


def split3(x):
    hi = x.astype(bf16).astype(f32)
    mid = (x - hi).astype(bf16).astype(f32)
    lo = (x - hi - mid).astype(bf16).astype(f32)
    return [hi, mid, lo]


def attend_kernel(
    me_ref, lens_ref, owner_ref, slot_ref, q_ref, nk_ref, nv_ref, k_hbm, v_hbm, out_ref,
    k_buf, v_buf, hi_ref, lo_ref, val_ref, key_ref, sems,
):
    requests, max_pages = owner_ref.shape
    rows, dim = q_ref.shape
    heads = rows // requests
    tokens = k_buf.shape[0]
    page = tokens // (SIDE * SIDE)
    steps = tokens // CHUNK
    copies = []
    for c in range(steps):
        part = pl.ds(c * CHUNK, CHUNK)
        pair = (
            pltpu.make_async_copy(k_hbm.at[part], k_buf.at[part], sems.at[0, c]),
            pltpu.make_async_copy(v_hbm.at[part], v_buf.at[part], sems.at[1, c]),
        )
        for copy in pair:
            copy.start()
        copies.append(pair)

    me = me_ref[0]
    row = iota((requests, 128), 0)
    lens = jnp.zeros((requests, 128), jnp.int32)
    for r in range(requests):
        lens = jnp.where(row == r, lens_ref[r], lens)
    lens = jnp.concatenate([lens] * (max_pages // 128), axis=1)
    live = jnp.clip(lens - page * iota(lens.shape, 1), 0, page)
    val = jnp.where(owner_ref[...] == me, iota(lens.shape, 0) * page + live, 0)
    hi_ref[...] = slot_ref[...] >> 5
    lo_ref[...] = slot_ref[...] & 31
    val_ref[...] = val.astype(f32)
    side = iota((SIDE, 128), 0)
    wide = BLOCK * SIDE
    table = jnp.zeros((wide, wide), f32)
    for j in range(max_pages // 128):
        lanes = slice(j * 128, (j + 1) * 128)
        for g in range(requests // BLOCK):
            put, at = [], []
            for r in range(g * BLOCK, (g + 1) * BLOCK):
                put.append(jnp.where(hi_ref[r : r + 1, lanes] == side, val_ref[r : r + 1, lanes], 0.0))
                at.append(jnp.where(lo_ref[r : r + 1, lanes] == side, 1.0, 0.0))
            table += dot_t(
                jnp.concatenate(put, axis=0).astype(bf16), jnp.concatenate(at, axis=0).astype(bf16)
            )
    same = iota((wide, wide), 0) // SIDE == iota((wide, wide), 1) // SIDE
    table = jnp.where(same, table, 0.0).astype(bf16)
    span = SIDE * page
    spread = jnp.where(
        iota((wide, span), 0) % SIDE == iota((wide, span), 1) // page, 1.0, 0.0
    ).astype(bf16)
    found = dot(table, spread)
    code = found[:SIDE]
    for b in range(1, BLOCK):
        code = code + found[b * SIDE : (b + 1) * SIDE]
    code = code.astype(jnp.int32) - 1
    key_ref[...] = jnp.where(iota(code.shape, 1) % page <= (code & (page - 1)), code >> 4, -1)

    turn_row = iota((rows, rows), 0)
    turn = jnp.where(
        iota((rows, rows), 1) == (turn_row % requests) * heads + turn_row // requests, 1.0, 0.0
    )
    q = dot(turn.astype(bf16), q_ref[...]).astype(bf16)
    scale = math.log2(math.e) / math.sqrt(dim)
    per = CHUNK // span
    wanted = iota((requests, span), 0)

    def scores(c):
        parts = []
        for i in range(per):
            s = dot_t(q, k_buf[c * CHUNK + i * span : c * CHUNK + (i + 1) * span, :])
            key = key_ref[c * per + i : c * per + i + 1, :]
            bias = jnp.where(key == wanted, 0.0, masked)
            parts.append(s + jnp.concatenate([bias] * heads, axis=0))
        return parts

    top = jnp.full((rows, 1), lowest, f32)
    total = jnp.zeros((rows, 1), f32)
    out = jnp.zeros((rows, dim), f32)
    copies[0][0].wait()
    now = scores(0)
    for c in range(steps):
        if c + 1 < steps:
            copies[c + 1][0].wait()
        copies[c][1].wait()
        after = scores(c + 1) if c + 1 < steps else None
        highest = now[0]
        for s in now[1:]:
            highest = jnp.maximum(highest, s)
        new_top = jnp.maximum(top, jnp.max(highest, axis=1, keepdims=True))
        keep = jnp.exp2((top - new_top) * scale)
        out = out * keep
        summed = None
        for i, s in enumerate(now):
            p = jnp.exp2((s - new_top) * scale)
            summed = p if summed is None else summed + p
            v = v_buf[c * CHUNK + i * span : c * CHUNK + (i + 1) * span, :]
            out = out + dot(p.astype(bf16), v)
        total = total * keep + jnp.sum(summed, axis=1, keepdims=True)
        top = new_top
        now = after

    nk = jnp.concatenate([nk_ref[...].astype(f32)] * heads, axis=0)
    nv = jnp.concatenate([nv_ref[...].astype(f32)] * heads, axis=0)
    self_score = jnp.sum(q.astype(f32) * nk, axis=1, keepdims=True)
    self_score = jnp.where(me == 0, self_score, masked)
    new_top = jnp.maximum(top, self_score)
    keep = jnp.exp2((top - new_top) * scale)
    take = jnp.exp2((self_score - new_top) * scale)
    out = out * keep + take * nv
    total = total * keep + take

    lane = iota((rows, 128), 1)
    group = (iota((rows, 128), 0) // requests) % 3
    meta = jnp.zeros((rows, 128), f32)
    for i, part in enumerate(split3(new_top) + split3(total)):
        meta = jnp.where(lane == 6 * group + i, part, meta)
    both = jnp.concatenate([out.astype(bf16), meta.astype(bf16)], axis=0)
    sent = out_ref.shape[0]
    to = iota((sent, 2 * rows), 0)
    source = iota((sent, 2 * rows), 1)
    inner = jnp.where(source < rows, source, source - rows)
    flat = (inner % requests) * heads + inner // requests
    data = (source < rows) & (to % 4 < 3) & (flat == (to // 4) * 3 + to % 4)
    head_row = (source >= rows) & (to % 4 == 3) & (flat // 3 == to // 4)
    pick = jnp.where(data, 1.0, jnp.where(head_row, 1.0, 0.0)).astype(bf16)
    out_ref[...] = dot(pick, both).astype(bf16)


def near_kernel(got_ref, out_ref, *, scale):
    sent = got_ref.shape[0]
    blocks = sent // (4 * NEAR)
    mine = 3 * blocks
    kept = out_ref.shape[1]
    got = got_ref[...]
    height = 2 * NEAR * kept
    to = iota((height, sent), 0)
    source = iota((height, sent), 1)
    line = to % kept
    near = (to // kept) % NEAR
    base = (line // 3) * (4 * NEAR) + near * 4
    wanted = jnp.where(to < NEAR * kept, base + line % 3, base + 3)
    pick = jnp.where((source == wanted) & (line < mine), 1.0, 0.0).astype(bf16)
    all_rows = dot(pick, got)
    lane = iota((kept, 128), 1)
    line = iota((kept, 128), 0)
    first = 6 * (line % 3)
    outs, tops, totals = [], [], []
    for b in range(NEAR):
        outs.append(all_rows[b * kept : (b + 1) * kept])
        meta = all_rows[(NEAR + b) * kept : (NEAR + b + 1) * kept]
        is_top = (lane >= first) & (lane < first + 3)
        is_total = (lane >= first + 3) & (lane < first + 6)
        tops.append(jnp.sum(jnp.where(is_top, meta, 0.0), axis=1, keepdims=True))
        totals.append(jnp.sum(jnp.where(is_total, meta, 0.0), axis=1, keepdims=True))
    top = tops[0]
    for t in tops[1:]:
        top = jnp.maximum(top, t)
    out = jnp.zeros((kept, 128), f32)
    total = jnp.zeros((kept, 1), f32)
    for b in range(NEAR):
        factor = jnp.exp2((tops[b] - top) * scale)
        out = out + factor * outs[b]
        total = total + factor * totals[b]
    for i, part in enumerate(split3(top) + split3(total)):
        across = jnp.sum(jnp.where(lane == line, part, 0.0), axis=0, keepdims=True)
        out = jnp.where(line == mine + i, across, out)
    out = out.astype(bf16)
    for d in range(out_ref.shape[0]):
        out_ref[d] = out


def project_kernel(got_ref, w_hbm, out_ref, w_buf, flat_ref, sems, *, scale):
    peers, kept, dim = got_ref.shape
    far = peers // NEAR
    mine = kept - 8
    inner = w_hbm.shape[0]
    piece = inner // W_CHUNKS
    copies = []
    for c in range(W_CHUNKS):
        part = pl.ds(c * piece, piece)
        copy = pltpu.make_async_copy(w_hbm.at[part], w_buf.at[part], sems.at[c])
        copy.start()
        copies.append(copy)
    flat_ref[...] = jnp.zeros(flat_ref.shape, f32)
    lane = iota((kept, 128), 1)
    line = iota((kept, 128), 0)
    for b in range(NEAR):
        outs, tops, totals = [], [], []
        for a in range(far):
            x = got_ref[a * NEAR + b].astype(f32)
            head = x[mine : mine + 8]
            top = head[0:1] + head[1:2] + head[2:3]
            total = head[3:4] + head[4:5] + head[5:6]
            outs.append(x)
            tops.append(jnp.sum(jnp.where(lane == line, top, 0.0), axis=1, keepdims=True))
            totals.append(jnp.sum(jnp.where(lane == line, total, 0.0), axis=1, keepdims=True))
        top = tops[0]
        for t in tops[1:]:
            top = jnp.maximum(top, t)
        out = jnp.zeros((kept, dim), f32)
        total = jnp.zeros((kept, 1), f32)
        for a in range(far):
            factor = jnp.exp2((tops[a] - top) * scale)
            out = out + factor * outs[a]
            total = total + factor * totals[a]
        attended = out / total
        halves = NEAR // 2
        request, half = b // halves, b % halves
        for i in range(mine):
            at = ((i // 3) * 3 * halves + half * 3 + i % 3) * dim
            flat_ref[request : request + 1, at : at + dim] = attended[i : i + 1]
    acc = jnp.zeros((8, w_hbm.shape[1]), f32)
    for c in range(W_CHUNKS):
        copies[c].wait()
        lhs = flat_ref[:, c * piece : (c + 1) * piece].astype(bf16)
        acc = acc + dot(lhs, w_buf[c * piece : (c + 1) * piece, :])
    out_ref[...] = acc[: out_ref.shape[0]].astype(bf16)


VMEM = pl.BlockSpec(memory_space=pltpu.VMEM)
SMEM = pl.BlockSpec(memory_space=pltpu.SMEM)
ANY = pl.BlockSpec(memory_space=pl.ANY)


def local(
    queries, k_cache, v_cache, new_key, new_value, ctx_lens, page_owner, page_slot, out_weight,
    interpret=False,
):
    _, slots, page, dim = k_cache.shape
    requests, heads, _ = queries.shape
    tokens = slots * page
    rows = requests * heads
    me = lax.axis_index(("far", "near")).astype(jnp.int32).reshape(1)
    sent = rows // 3 * 4
    scale = math.log2(math.e) / math.sqrt(dim)
    partial = attend_call(
        me, ctx_lens, page_owner, page_slot, queries.reshape(rows, dim), new_key[0], new_value[0],
        k_cache.reshape(tokens, dim), v_cache.reshape(tokens, dim), sent, interpret,
    )
    got = lax.all_to_all(partial, ("heads", "near"), 0, 0, tiled=True)
    peers = lax.axis_size("far") * lax.axis_size("near")
    merged = near_call(got, peers, scale, interpret)
    everything = lax.all_to_all(merged, ("far", "near"), 0, 0, tiled=True)
    mine = requests // lax.axis_size("heads")
    return project_call(everything, out_weight, mine, scale, interpret)


def attend_call(me, lens, owner, slot, q, nk, nv, k, v, sent, interpret):
    tokens, dim = k.shape
    requests, max_pages = owner.shape
    return pl.pallas_call(
        attend_kernel,
        out_shape=jax.ShapeDtypeStruct((sent, dim), bf16),
        in_specs=[SMEM, SMEM, VMEM, VMEM, VMEM, VMEM, VMEM, ANY, ANY],
        out_specs=VMEM,
        scratch_shapes=[
            pltpu.VMEM((tokens, dim), bf16),
            pltpu.VMEM((tokens, dim), bf16),
            pltpu.VMEM((requests, max_pages), jnp.int32),
            pltpu.VMEM((requests, max_pages), jnp.int32),
            pltpu.VMEM((requests, max_pages), f32),
            pltpu.VMEM((SIDE, tokens // SIDE), jnp.int32),
            pltpu.SemaphoreType.DMA((2, tokens // CHUNK)),
        ],
        interpret=interpret,
        name="attend",
    )(me, lens, owner, slot, q, nk, nv, k, v)


def near_call(got, peers, scale, interpret):
    sent, dim = got.shape
    kept = sent // (4 * NEAR) * 3 + 8
    return pl.pallas_call(
        lambda *refs: near_kernel(*refs, scale=scale),
        out_shape=jax.ShapeDtypeStruct((peers, kept, dim), bf16),
        in_specs=[VMEM],
        out_specs=VMEM,
        interpret=interpret,
        name="near",
    )(got)


def project_call(everything, w, mine, scale, interpret):
    inner, features = w.shape
    return pl.pallas_call(
        lambda *refs: project_kernel(*refs, scale=scale),
        out_shape=jax.ShapeDtypeStruct((mine, features), bf16),
        in_specs=[VMEM, ANY],
        out_specs=VMEM,
        scratch_shapes=[
            pltpu.VMEM((inner, features), bf16),
            pltpu.VMEM((8, inner), f32),
            pltpu.SemaphoreType.DMA((W_CHUNKS,)),
        ],
        interpret=interpret,
        name="project",
    )(everything, w)


def solution(mesh):
    torus = Mesh(
        mesh.devices.reshape(
            mesh.shape["group"], mesh.shape["pages"] // NEAR, NEAR, mesh.shape["heads"]
        ),
        ("group", "far", "near", "heads"),
    )
    pages = ("far", "near")
    in_specs = (
        P("group", "heads", None),
        P("heads", ("group", *pages), None, None),
        P("heads", ("group", *pages), None, None),
        P("heads", "group", None),
        P("heads", "group", None),
        P("group"),
        P("group", None),
        P("group", None),
        P(None, pages),
    )
    out_specs = P(("group", "heads"), pages)
    return jax.shard_map(local, mesh=torus, in_specs=in_specs, out_specs=out_specs, check_vma=False)
```

```python
import math

import jax
import jax.numpy as jnp
from jax import lax
from jax.experimental import pallas as pl
from jax.experimental.pallas import tpu as pltpu
from jax.sharding import Mesh
from jax.sharding import PartitionSpec as P

NEAR = 4
CHUNK = 4096
SIDE = 32
BLOCK = 8

f32 = jnp.float32
bf16 = jnp.bfloat16
masked = -1e30
lowest = -1e29


def iota(shape, dim):
    return lax.broadcasted_iota(jnp.int32, shape, dim)


def dot(a, b):
    return jnp.dot(a, b, preferred_element_type=f32)


def dot_t(a, b):
    return lax.dot_general(a, b, (((1,), (1,)), ((), ())), preferred_element_type=f32)


def split3(x):
    hi = x.astype(bf16).astype(f32)
    mid = (x - hi).astype(bf16).astype(f32)
    lo = (x - hi - mid).astype(bf16).astype(f32)
    return [hi, mid, lo]


def attend_kernel(
    lens_hbm, owner_hbm, slot_hbm, q_hbm, nk_hbm, nv_hbm, k_hbm, v_hbm, out_ref,
    lens_ref, owner_ref, slot_ref, q_ref, nk_ref, nv_ref,
    k_buf, v_buf, hi_ref, lo_ref, val_ref, key_ref, small_sems, sems, *, position,
):
    requests, max_pages = owner_ref.shape
    rows, dim = q_ref.shape
    heads = rows // requests
    tokens = k_buf.shape[0]
    page = tokens // (SIDE * SIDE)
    steps = tokens // CHUNK
    copies = []
    small = [
        pltpu.make_async_copy(source, target, small_sems.at[i])
        for i, (source, target) in enumerate(
            [
                (lens_hbm, lens_ref), (owner_hbm, owner_ref), (slot_hbm, slot_ref),
                (q_hbm, q_ref), (nk_hbm, nk_ref), (nv_hbm, nv_ref),
            ]
        )
    ]
    for copy in small:
        copy.start()
    for copy in small:
        copy.wait()
    for c in range(steps):
        part = pl.ds(c * CHUNK, CHUNK)
        pair = (
            pltpu.make_async_copy(k_hbm.at[part], k_buf.at[part], sems.at[0, c]),
            pltpu.make_async_copy(v_hbm.at[part], v_buf.at[part], sems.at[1, c]),
        )
        for copy in pair:
            copy.start()
        copies.append(pair)

    me = position()
    row = iota((requests, 128), 0)
    lens = jnp.zeros((requests, 128), jnp.int32)
    for r in range(requests):
        lens = jnp.where(row == r, lens_ref[r], lens)
    lens = jnp.concatenate([lens] * (max_pages // 128), axis=1)
    live = jnp.clip(lens - page * iota(lens.shape, 1), 0, page)
    val = jnp.where(owner_ref[...] == me, iota(lens.shape, 0) * page + live, 0)
    hi_ref[...] = slot_ref[...] >> 5
    lo_ref[...] = slot_ref[...] & 31
    val_ref[...] = val.astype(f32)
    side = iota((SIDE, 128), 0)
    wide = BLOCK * SIDE
    table = jnp.zeros((wide, wide), f32)
    for j in range(max_pages // 128):
        lanes = slice(j * 128, (j + 1) * 128)
        for g in range(requests // BLOCK):
            put, at = [], []
            for r in range(g * BLOCK, (g + 1) * BLOCK):
                put.append(jnp.where(hi_ref[r : r + 1, lanes] == side, val_ref[r : r + 1, lanes], 0.0))
                at.append(jnp.where(lo_ref[r : r + 1, lanes] == side, 1.0, 0.0))
            table += dot_t(
                jnp.concatenate(put, axis=0).astype(bf16), jnp.concatenate(at, axis=0).astype(bf16)
            )
    same = iota((wide, wide), 0) // SIDE == iota((wide, wide), 1) // SIDE
    table = jnp.where(same, table, 0.0).astype(bf16)
    span = SIDE * page
    spread = jnp.where(
        iota((wide, span), 0) % SIDE == iota((wide, span), 1) // page, 1.0, 0.0
    ).astype(bf16)
    found = dot(table, spread)
    code = found[:SIDE]
    for b in range(1, BLOCK):
        code = code + found[b * SIDE : (b + 1) * SIDE]
    code = code.astype(jnp.int32) - 1
    key_ref[...] = jnp.where(iota(code.shape, 1) % page <= (code & (page - 1)), code >> 4, -1)

    q = q_ref[...]
    scale = math.log2(math.e) / math.sqrt(dim)
    per = CHUNK // span
    wanted = iota((requests, span), 0)

    def scores(c):
        parts = []
        for i in range(per):
            s = dot_t(q, k_buf[c * CHUNK + i * span : c * CHUNK + (i + 1) * span, :])
            key = key_ref[c * per + i : c * per + i + 1, :]
            bias = jnp.where(key == wanted, 0.0, masked)
            parts.append(s + jnp.concatenate([bias] * heads, axis=0))
        return parts

    top = jnp.full((rows, 1), lowest, f32)
    total = jnp.zeros((rows, 1), f32)
    out = jnp.zeros((rows, dim), f32)
    copies[0][0].wait()
    now = scores(0)
    for c in range(steps):
        if c + 1 < steps:
            copies[c + 1][0].wait()
        copies[c][1].wait()
        after = scores(c + 1) if c + 1 < steps else None
        highest = now[0]
        for s in now[1:]:
            highest = jnp.maximum(highest, s)
        new_top = jnp.maximum(top, jnp.max(highest, axis=1, keepdims=True))
        keep = jnp.exp2((top - new_top) * scale)
        out = out * keep
        summed = None
        for i, s in enumerate(now):
            p = jnp.exp2((s - new_top) * scale)
            summed = p if summed is None else summed + p
            v = v_buf[c * CHUNK + i * span : c * CHUNK + (i + 1) * span, :]
            out = out + dot(p.astype(bf16), v)
        total = total * keep + jnp.sum(summed, axis=1, keepdims=True)
        top = new_top
        now = after

    nk = jnp.concatenate([nk_ref[...].astype(f32)] * heads, axis=0)
    nv = jnp.concatenate([nv_ref[...].astype(f32)] * heads, axis=0)
    self_score = jnp.sum(q.astype(f32) * nk, axis=1, keepdims=True)
    self_score = jnp.where(me == 0, self_score, masked)
    new_top = jnp.maximum(top, self_score)
    keep = jnp.exp2((top - new_top) * scale)
    take = jnp.exp2((self_score - new_top) * scale)
    out = out * keep + take * nv
    total = total * keep + take

    lane = iota((rows, 128), 1)
    group = (iota((rows, 128), 0) // requests) % 3
    meta = jnp.zeros((rows, 128), f32)
    for i, part in enumerate(split3(new_top) + split3(total)):
        meta = jnp.where(lane == 6 * group + i, part, meta)
    both = jnp.concatenate([out.astype(bf16), meta.astype(bf16)], axis=0)
    sent = out_ref.shape[0]
    to = iota((sent, 2 * rows), 0)
    source = iota((sent, 2 * rows), 1)
    inner = jnp.where(source < rows, source, source - rows)
    flat = (inner % requests) * heads + inner // requests
    data = (source < rows) & (to % 4 < 3) & (flat == (to // 4) * 3 + to % 4)
    head_row = (source >= rows) & (to % 4 == 3) & (flat // 3 == to // 4)
    pick = jnp.where(data, 1.0, jnp.where(head_row, 1.0, 0.0)).astype(bf16)
    out_ref[...] = dot(pick, both).astype(bf16)


def near_kernel(got_ref, out_ref, *, scale):
    sent = got_ref.shape[0]
    blocks = sent // (4 * NEAR)
    mine = 3 * blocks
    kept = out_ref.shape[1]
    got = got_ref[...]
    height = 2 * NEAR * kept
    to = iota((height, sent), 0)
    source = iota((height, sent), 1)
    line = to % kept
    near = (to // kept) % NEAR
    base = (line // 3) * (4 * NEAR) + near * 4
    wanted = jnp.where(to < NEAR * kept, base + line % 3, base + 3)
    pick = jnp.where((source == wanted) & (line < mine), 1.0, 0.0).astype(bf16)
    all_rows = dot(pick, got)
    lane = iota((kept, 128), 1)
    line = iota((kept, 128), 0)
    first = 6 * (line % 3)
    outs, tops, totals = [], [], []
    for b in range(NEAR):
        outs.append(all_rows[b * kept : (b + 1) * kept])
        meta = all_rows[(NEAR + b) * kept : (NEAR + b + 1) * kept]
        is_top = (lane >= first) & (lane < first + 3)
        is_total = (lane >= first + 3) & (lane < first + 6)
        tops.append(jnp.sum(jnp.where(is_top, meta, 0.0), axis=1, keepdims=True))
        totals.append(jnp.sum(jnp.where(is_total, meta, 0.0), axis=1, keepdims=True))
    top = tops[0]
    for t in tops[1:]:
        top = jnp.maximum(top, t)
    out = jnp.zeros((kept, 128), f32)
    total = jnp.zeros((kept, 1), f32)
    for b in range(NEAR):
        factor = jnp.exp2((tops[b] - top) * scale)
        out = out + factor * outs[b]
        total = total + factor * totals[b]
    for i, part in enumerate(split3(top) + split3(total)):
        across = jnp.sum(jnp.where(lane == line, part, 0.0), axis=0, keepdims=True)
        out = jnp.where(line == mine + i, across, out)
    out = out.astype(bf16)
    for d in range(out_ref.shape[0]):
        out_ref[d] = out


def project_kernel(got_ref, w_ref, out_ref, flat_ref, *, scale):
    peers, kept, dim = got_ref.shape
    far = peers // NEAR
    mine = kept - 8
    flat_ref[...] = jnp.zeros(flat_ref.shape, f32)
    lane = iota((kept, 128), 1)
    line = iota((kept, 128), 0)
    for b in range(NEAR):
        outs, tops, totals = [], [], []
        for a in range(far):
            x = got_ref[a * NEAR + b].astype(f32)
            head = x[mine : mine + 8]
            top = head[0:1] + head[1:2] + head[2:3]
            total = head[3:4] + head[4:5] + head[5:6]
            outs.append(x)
            tops.append(jnp.sum(jnp.where(lane == line, top, 0.0), axis=1, keepdims=True))
            totals.append(jnp.sum(jnp.where(lane == line, total, 0.0), axis=1, keepdims=True))
        top = tops[0]
        for t in tops[1:]:
            top = jnp.maximum(top, t)
        out = jnp.zeros((kept, dim), f32)
        total = jnp.zeros((kept, 1), f32)
        for a in range(far):
            factor = jnp.exp2((tops[a] - top) * scale)
            out = out + factor * outs[a]
            total = total + factor * totals[a]
        attended = out / total
        halves = NEAR // 2
        request, half = b // halves, b % halves
        for i in range(mine):
            at = ((i // 3) * 3 * halves + half * 3 + i % 3) * dim
            flat_ref[request : request + 1, at : at + dim] = attended[i : i + 1]
    projected = dot(flat_ref[...].astype(bf16), w_ref[...])
    out_ref[...] = projected[: out_ref.shape[0]].astype(bf16)


VMEM = pl.BlockSpec(memory_space=pltpu.VMEM)
ANY = pl.BlockSpec(memory_space=pl.ANY)


def local(
    queries, k_cache, v_cache, new_key, new_value, ctx_lens, page_owner, page_slot, out_weight,
    interpret=False,
):
    _, slots, page, dim = k_cache.shape
    requests, heads, _ = queries.shape
    tokens = slots * page
    rows = requests * heads
    sent = rows // 3 * 4
    scale = math.log2(math.e) / math.sqrt(dim)
    partial = attend_call(
        lambda: lax.axis_index(("far", "near")), ctx_lens, page_owner, page_slot, queries.transpose(1, 0, 2).reshape(rows, dim), new_key[0], new_value[0],
        k_cache.reshape(tokens, dim), v_cache.reshape(tokens, dim), sent, interpret,
    )
    partial, out_weight = lax.optimization_barrier((partial, out_weight))
    got = lax.all_to_all(partial, ("heads", "near"), 0, 0, tiled=True)
    peers = lax.axis_size("far") * lax.axis_size("near")
    merged = near_call(got, peers, scale, interpret)
    everything = lax.all_to_all(merged, ("far", "near"), 0, 0, tiled=True)
    mine = requests // lax.axis_size("heads")
    return project_call(everything, out_weight, mine, scale, interpret)


def in_hbm(x):
    return pltpu.with_memory_space_constraint(x, pltpu.HBM)


def attend_call(position, lens, owner, slot, q, nk, nv, k, v, sent, interpret):
    tokens, dim = k.shape
    requests, max_pages = owner.shape
    return pl.pallas_call(
        lambda *refs: attend_kernel(*refs, position=position),
        out_shape=jax.ShapeDtypeStruct((sent, dim), bf16),
        in_specs=[ANY] * 8,
        out_specs=VMEM,
        scratch_shapes=[
            pltpu.SMEM(lens.shape, lens.dtype),
            *(pltpu.VMEM(x.shape, x.dtype) for x in (owner, slot, q, nk, nv)),
            pltpu.VMEM((tokens, dim), bf16),
            pltpu.VMEM((tokens, dim), bf16),
            pltpu.VMEM((requests, max_pages), jnp.int32),
            pltpu.VMEM((requests, max_pages), jnp.int32),
            pltpu.VMEM((requests, max_pages), f32),
            pltpu.VMEM((SIDE, tokens // SIDE), jnp.int32),
            pltpu.SemaphoreType.DMA((6,)),
            pltpu.SemaphoreType.DMA((2, tokens // CHUNK)),
        ],
        compiler_params=pltpu.CompilerParams(vmem_limit_bytes=24 << 20),
        interpret=interpret,
        name="attend",
    )(*(in_hbm(x) for x in (lens, owner, slot, q, nk, nv, k, v)))


def near_call(got, peers, scale, interpret):
    sent, dim = got.shape
    kept = sent // (4 * NEAR) * 3 + 8
    return pl.pallas_call(
        lambda *refs: near_kernel(*refs, scale=scale),
        out_shape=jax.ShapeDtypeStruct((peers, kept, dim), bf16),
        in_specs=[VMEM],
        out_specs=VMEM,
        compiler_params=pltpu.CompilerParams(vmem_limit_bytes=4 << 20),
        interpret=interpret,
        name="near",
    )(got)


def project_call(everything, w, mine, scale, interpret):
    inner, features = w.shape
    return pl.pallas_call(
        lambda *refs: project_kernel(*refs, scale=scale),
        out_shape=jax.ShapeDtypeStruct((mine, features), bf16),
        in_specs=[VMEM, VMEM],
        out_specs=VMEM,
        scratch_shapes=[pltpu.VMEM((8, inner), f32)],
        compiler_params=pltpu.CompilerParams(vmem_limit_bytes=8 << 20),
        interpret=interpret,
        name="project",
    )(everything, pltpu.with_memory_space_constraint(w, pltpu.VMEM))


def solution(mesh):
    torus = Mesh(
        mesh.devices.reshape(
            mesh.shape["group"], mesh.shape["pages"] // NEAR, NEAR, mesh.shape["heads"]
        ),
        ("group", "far", "near", "heads"),
    )
    pages = ("far", "near")
    in_specs = (
        P("group", "heads", None),
        P("heads", ("group", *pages), None, None),
        P("heads", ("group", *pages), None, None),
        P("heads", "group", None),
        P("heads", "group", None),
        P("group"),
        P("group", None),
        P("group", None),
        P(None, pages),
    )
    out_specs = P(("group", "heads"), pages)
    return jax.shard_map(local, mesh=torus, in_specs=in_specs, out_specs=out_specs, check_vma=False)
```

```python
import math

import jax
import jax.numpy as jnp
from jax import lax
from jax.experimental import pallas as pl
from jax.experimental.pallas import tpu as pltpu
from jax.sharding import Mesh
from jax.sharding import PartitionSpec as P

NEAR = 4
CHUNK = 4096
SIDE = 32
BLOCK = 4
ENTRIES = 256

f32 = jnp.float32
bf16 = jnp.bfloat16
masked = -1e30
lowest = -1e29


def iota(shape, dim):
    return lax.broadcasted_iota(jnp.int32, shape, dim)


def dot(a, b):
    return jnp.dot(a, b, preferred_element_type=f32)


def dot_t(a, b):
    return lax.dot_general(a, b, (((1,), (1,)), ((), ())), preferred_element_type=f32)


def split3(x):
    hi = x.astype(bf16).astype(f32)
    mid = (x - hi).astype(bf16).astype(f32)
    lo = (x - hi - mid).astype(bf16).astype(f32)
    return [hi, mid, lo]


def attend_kernel(
    lens_hbm, owner_hbm, slot_hbm, q_hbm, nk_hbm, nv_hbm, k_hbm, v_hbm, out_ref,
    lens_ref, owner_ref, slot_ref, q_ref, nk_ref, nv_ref,
    k_buf, v_buf, hi_ref, lo_ref, val_ref, key_ref, small_sems, sems, *, position,
):
    requests, max_pages = owner_ref.shape
    rows, dim = q_ref.shape
    heads = rows // requests
    tokens = k_buf.shape[0]
    page = tokens // (SIDE * SIDE)
    steps = tokens // CHUNK
    copies = []
    small = [
        pltpu.make_async_copy(source, target, small_sems.at[i])
        for i, (source, target) in enumerate(
            [
                (lens_hbm, lens_ref), (owner_hbm, owner_ref), (slot_hbm, slot_ref),
                (q_hbm, q_ref), (nk_hbm, nk_ref), (nv_hbm, nv_ref),
            ]
        )
    ]
    for copy in small:
        copy.start()
    for copy in small:
        copy.wait()
    for c in range(steps):
        part = pl.ds(c * CHUNK, CHUNK)
        pair = (
            pltpu.make_async_copy(k_hbm.at[part], k_buf.at[part], sems.at[0, c]),
            pltpu.make_async_copy(v_hbm.at[part], v_buf.at[part], sems.at[1, c]),
        )
        for copy in pair:
            copy.start()
        copies.append(pair)

    me = position()
    row = iota((requests, 128), 0)
    lens = jnp.zeros((requests, 128), jnp.int32)
    for r in range(requests):
        lens = jnp.where(row == r, lens_ref[r], lens)
    lens = jnp.concatenate([lens] * (max_pages // 128), axis=1)
    live = jnp.clip(lens - page * iota(lens.shape, 1), 0, page)
    val = jnp.where(owner_ref[...] == me, iota(lens.shape, 0) * page + live, 0)
    hi_ref[...] = slot_ref[...] >> 5
    lo_ref[...] = slot_ref[...] & 31
    val_ref[...] = val.astype(f32)
    side = iota((SIDE, ENTRIES), 0)
    wide = BLOCK * SIDE
    table = jnp.zeros((wide, wide), f32)
    for j in range(max_pages // ENTRIES):
        lanes = slice(j * ENTRIES, (j + 1) * ENTRIES)
        for g in range(requests // BLOCK):
            put, at = [], []
            for r in range(g * BLOCK, (g + 1) * BLOCK):
                put.append(jnp.where(hi_ref[r : r + 1, lanes] == side, val_ref[r : r + 1, lanes], 0.0))
                at.append(jnp.where(lo_ref[r : r + 1, lanes] == side, 1.0, 0.0))
            table += dot_t(
                jnp.concatenate(put, axis=0).astype(bf16), jnp.concatenate(at, axis=0).astype(bf16)
            )
    same = iota((wide, wide), 0) // SIDE == iota((wide, wide), 1) // SIDE
    table = jnp.where(same, table, 0.0).astype(bf16)
    span = SIDE * page
    spread = jnp.where(
        iota((wide, span), 0) % SIDE == iota((wide, span), 1) // page, 1.0, 0.0
    ).astype(bf16)
    found = dot(table, spread)
    code = found[:SIDE]
    for b in range(1, BLOCK):
        code = code + found[b * SIDE : (b + 1) * SIDE]
    code = code.astype(jnp.int32) - 1
    key_ref[...] = jnp.where(iota(code.shape, 1) % page <= (code & (page - 1)), code >> 4, -1)

    q = q_ref[...]
    scale = math.log2(math.e) / math.sqrt(dim)
    per = CHUNK // span
    wanted = iota((requests, span), 0)

    def scores(c):
        parts = []
        for i in range(per):
            s = dot_t(q, k_buf[c * CHUNK + i * span : c * CHUNK + (i + 1) * span, :])
            key = key_ref[c * per + i : c * per + i + 1, :]
            bias = jnp.where(key == wanted, 0.0, masked)
            parts.append(s + jnp.concatenate([bias] * heads, axis=0))
        return parts

    top = jnp.full((rows, 1), lowest, f32)
    total = jnp.zeros((rows, 1), f32)
    out = jnp.zeros((rows, dim), f32)
    copies[0][0].wait()
    now = scores(0)
    for c in range(steps):
        if c + 1 < steps:
            copies[c + 1][0].wait()
        copies[c][1].wait()
        after = scores(c + 1) if c + 1 < steps else None
        highest = now[0]
        for s in now[1:]:
            highest = jnp.maximum(highest, s)
        new_top = jnp.maximum(top, jnp.max(highest, axis=1, keepdims=True))
        keep = jnp.exp2((top - new_top) * scale)
        out = out * keep
        summed = None
        for i, s in enumerate(now):
            p = jnp.exp2((s - new_top) * scale)
            summed = p if summed is None else summed + p
            v = v_buf[c * CHUNK + i * span : c * CHUNK + (i + 1) * span, :]
            out = out + dot(p.astype(bf16), v)
        total = total * keep + jnp.sum(summed, axis=1, keepdims=True)
        top = new_top
        now = after

    nk = jnp.concatenate([nk_ref[...].astype(f32)] * heads, axis=0)
    nv = jnp.concatenate([nv_ref[...].astype(f32)] * heads, axis=0)
    self_score = jnp.sum(q.astype(f32) * nk, axis=1, keepdims=True)
    self_score = jnp.where(me == 0, self_score, masked)
    new_top = jnp.maximum(top, self_score)
    keep = jnp.exp2((top - new_top) * scale)
    take = jnp.exp2((self_score - new_top) * scale)
    out = out * keep + take * nv
    total = total * keep + take

    lane = iota((rows, 128), 1)
    group = (iota((rows, 128), 0) // requests) % 3
    meta = jnp.zeros((rows, 128), f32)
    for i, part in enumerate(split3(new_top) + split3(total)):
        meta = jnp.where(lane == 6 * group + i, part, meta)
    both = jnp.concatenate([out.astype(bf16), meta.astype(bf16)], axis=0)
    sent = out_ref.shape[0]
    to = iota((sent, 2 * rows), 0)
    source = iota((sent, 2 * rows), 1)
    inner = jnp.where(source < rows, source, source - rows)
    flat = (inner % requests) * heads + inner // requests
    data = (source < rows) & (to % 4 < 3) & (flat == (to // 4) * 3 + to % 4)
    head_row = (source >= rows) & (to % 4 == 3) & (flat // 3 == to // 4)
    pick = jnp.where(data, 1.0, jnp.where(head_row, 1.0, 0.0)).astype(bf16)
    out_ref[...] = dot(pick, both).astype(bf16)


def near_kernel(got_ref, out_ref, *, scale):
    sent = got_ref.shape[0]
    blocks = sent // (4 * NEAR)
    mine = 3 * blocks
    kept = mine + 8
    got = got_ref[...]
    height = 2 * NEAR * kept
    to = iota((height, sent), 0)
    source = iota((height, sent), 1)
    line = to % kept
    near = (to // kept) % NEAR
    base = (line // 3) * (4 * NEAR) + near * 4
    wanted = jnp.where(to < NEAR * kept, base + line % 3, base + 3)
    pick = jnp.where((source == wanted) & (line < mine), 1.0, 0.0).astype(bf16)
    all_rows = dot(pick, got)
    lane = iota((kept, 128), 1)
    line = iota((kept, 128), 0)
    first = 6 * (line % 3)
    outs, tops, totals = [], [], []
    for b in range(NEAR):
        outs.append(all_rows[b * kept : (b + 1) * kept])
        meta = all_rows[(NEAR + b) * kept : (NEAR + b + 1) * kept]
        is_top = (lane >= first) & (lane < first + 3)
        is_total = (lane >= first + 3) & (lane < first + 6)
        tops.append(jnp.sum(jnp.where(is_top, meta, 0.0), axis=1, keepdims=True))
        totals.append(jnp.sum(jnp.where(is_total, meta, 0.0), axis=1, keepdims=True))
    top = tops[0]
    for t in tops[1:]:
        top = jnp.maximum(top, t)
    out = jnp.zeros((kept, 128), f32)
    total = jnp.zeros((kept, 1), f32)
    for b in range(NEAR):
        factor = jnp.exp2((tops[b] - top) * scale)
        out = out + factor * outs[b]
        total = total + factor * totals[b]
    meta = jnp.zeros((kept, 128), f32)
    for i, part in enumerate(split3(top) + split3(total)[:2]):
        meta = jnp.where((lane == line + i * mine) & (line < mine), part, meta)
    out = jnp.where(line == mine, jnp.sum(meta, axis=0, keepdims=True), out)
    block = mine + 2
    out = out.astype(bf16)[:block]
    for d in range(out_ref.shape[0] // block):
        out_ref[d * block : (d + 1) * block, :] = out


def project_kernel(got_ref, w_ref, out_ref, flat_ref, *, scale, block):
    total_rows, dim = got_ref.shape
    far = total_rows // block // NEAR
    mine = block - 2
    flat_ref[...] = jnp.zeros(flat_ref.shape, f32)
    lane = iota((mine, 128), 1)
    line = iota((mine, 128), 0)
    is_top = (lane % mine == line) & (lane < 3 * mine)
    is_total = (lane % mine == line) & (lane >= 3 * mine) & (lane < 5 * mine)
    for b in range(NEAR):
        outs, tops, totals = [], [], []
        for a in range(far):
            first = (a * NEAR + b) * block
            x = got_ref[first : first + block, :].astype(f32)
            head = x[mine : mine + 1]
            outs.append(x[:mine])
            tops.append(jnp.sum(jnp.where(is_top, head, 0.0), axis=1, keepdims=True))
            totals.append(jnp.sum(jnp.where(is_total, head, 0.0), axis=1, keepdims=True))
        top = tops[0]
        for t in tops[1:]:
            top = jnp.maximum(top, t)
        out = jnp.zeros((mine, dim), f32)
        total = jnp.zeros((mine, 1), f32)
        for a in range(far):
            factor = jnp.exp2((tops[a] - top) * scale)
            out = out + factor * outs[a]
            total = total + factor * totals[a]
        attended = out / total
        halves = NEAR // 2
        request, half = b // halves, b % halves
        for i in range(mine):
            at = ((i // 3) * 3 * halves + half * 3 + i % 3) * dim
            flat_ref[request : request + 1, at : at + dim] = attended[i : i + 1]
    projected = dot(flat_ref[...].astype(bf16), w_ref[...])
    out_ref[...] = projected[: out_ref.shape[0]].astype(bf16)


VMEM = pl.BlockSpec(memory_space=pltpu.VMEM)
ANY = pl.BlockSpec(memory_space=pl.ANY)


def local(
    queries, k_cache, v_cache, new_key, new_value, ctx_lens, page_owner, page_slot, out_weight,
    interpret=False,
):
    _, slots, page, dim = k_cache.shape
    requests, heads, _ = queries.shape
    tokens = slots * page
    rows = requests * heads
    sent = rows // 3 * 4
    scale = math.log2(math.e) / math.sqrt(dim)
    partial = attend_call(
        lambda: lax.axis_index(("far", "near")), ctx_lens, page_owner, page_slot, queries.transpose(1, 0, 2).reshape(rows, dim), new_key[0], new_value[0],
        k_cache.reshape(tokens, dim), v_cache.reshape(tokens, dim), sent, interpret,
    )
    partial, out_weight = lax.optimization_barrier((partial, out_weight))
    got = lax.all_to_all(partial, ("heads", "near"), 0, 0, tiled=True)
    peers = lax.axis_size("far") * lax.axis_size("near")
    merged = near_call(got, peers, scale, interpret)
    block = merged.shape[0] // peers
    merged = merged.reshape(peers, block // 2, 2, dim)
    everything = lax.all_to_all(merged, ("far", "near"), 0, 0, tiled=True)
    everything = everything.reshape(peers * block, dim)
    mine = requests // lax.axis_size("heads")
    return project_call(everything, out_weight, mine, block, scale, interpret)


def in_hbm(x):
    return pltpu.with_memory_space_constraint(x, pltpu.HBM)


def attend_call(position, lens, owner, slot, q, nk, nv, k, v, sent, interpret):
    tokens, dim = k.shape
    requests, max_pages = owner.shape
    return pl.pallas_call(
        lambda *refs: attend_kernel(*refs, position=position),
        out_shape=jax.ShapeDtypeStruct((sent, dim), bf16),
        in_specs=[ANY] * 8,
        out_specs=VMEM,
        scratch_shapes=[
            pltpu.SMEM(lens.shape, lens.dtype),
            *(pltpu.VMEM(x.shape, x.dtype) for x in (owner, slot, q, nk, nv)),
            pltpu.VMEM((tokens, dim), bf16),
            pltpu.VMEM((tokens, dim), bf16),
            pltpu.VMEM((requests, max_pages), jnp.int32),
            pltpu.VMEM((requests, max_pages), jnp.int32),
            pltpu.VMEM((requests, max_pages), f32),
            pltpu.VMEM((SIDE, tokens // SIDE), jnp.int32),
            pltpu.SemaphoreType.DMA((6,)),
            pltpu.SemaphoreType.DMA((2, tokens // CHUNK)),
        ],
        compiler_params=pltpu.CompilerParams(vmem_limit_bytes=24 << 20),
        interpret=interpret,
        name="attend",
    )(*(in_hbm(x) for x in (lens, owner, slot, q, nk, nv, k, v)))


def near_call(got, peers, scale, interpret):
    sent, dim = got.shape
    block = sent // (4 * NEAR) * 3 + 2
    return pl.pallas_call(
        lambda *refs: near_kernel(*refs, scale=scale),
        out_shape=jax.ShapeDtypeStruct((peers * block, dim), bf16),
        in_specs=[VMEM],
        out_specs=VMEM,
        compiler_params=pltpu.CompilerParams(vmem_limit_bytes=4 << 20),
        interpret=interpret,
        name="near",
    )(got)


def project_call(everything, w, mine, block, scale, interpret):
    inner, features = w.shape
    return pl.pallas_call(
        lambda *refs: project_kernel(*refs, scale=scale, block=block),
        out_shape=jax.ShapeDtypeStruct((mine, features), bf16),
        in_specs=[VMEM, VMEM],
        out_specs=VMEM,
        scratch_shapes=[pltpu.VMEM((8, inner), f32)],
        compiler_params=pltpu.CompilerParams(vmem_limit_bytes=8 << 20),
        interpret=interpret,
        name="project",
    )(everything, pltpu.with_memory_space_constraint(w, pltpu.VMEM))


def solution(mesh):
    torus = Mesh(
        mesh.devices.reshape(
            mesh.shape["group"], mesh.shape["pages"] // NEAR, NEAR, mesh.shape["heads"]
        ),
        ("group", "far", "near", "heads"),
    )
    pages = ("far", "near")
    in_specs = (
        P("group", "heads", None),
        P("heads", ("group", *pages), None, None),
        P("heads", ("group", *pages), None, None),
        P("heads", "group", None),
        P("heads", "group", None),
        P("group"),
        P("group", None),
        P("group", None),
        P(None, pages),
    )
    out_specs = P(("group", "heads"), pages)
    return jax.shard_map(local, mesh=torus, in_specs=in_specs, out_specs=out_specs, check_vma=False)
```

```python
import math

import jax
import jax.numpy as jnp
from jax import lax
from jax.experimental import pallas as pl
from jax.experimental.pallas import tpu as pltpu
from jax.sharding import Mesh
from jax.sharding import PartitionSpec as P

NEAR = 4
CHUNK = 8192
STRIDE = 1024
SIDE = 32
BLOCK = 4
ENTRIES = 256

f32 = jnp.float32
bf16 = jnp.bfloat16
masked = -1e30
lowest = -1e29


def iota(shape, dim):
    return lax.broadcasted_iota(jnp.int32, shape, dim)


def dot(a, b):
    return jnp.dot(a, b, preferred_element_type=f32)


def dot_t(a, b):
    return lax.dot_general(a, b, (((1,), (1,)), ((), ())), preferred_element_type=f32)


def split3(x):
    hi = x.astype(bf16).astype(f32)
    mid = (x - hi).astype(bf16).astype(f32)
    lo = (x - hi - mid).astype(bf16).astype(f32)
    return [hi, mid, lo]


def attend_kernel(
    lens_hbm, owner_hbm, slot_hbm, q_hbm, nk_hbm, nv_hbm, k_hbm, v_hbm, out_ref,
    lens_ref, owner_ref, slot_ref, q_ref, nk_ref, nv_ref,
    k_buf, v_buf, s_buf, hi_ref, lo_ref, val_ref, key_ref, small_sems, sems, *, position,
):
    requests, max_pages = owner_ref.shape
    rows, dim = q_ref.shape
    heads = rows // requests
    tokens = k_buf.shape[0]
    page = tokens // (SIDE * SIDE)
    steps = tokens // CHUNK
    copies = []
    small = [
        pltpu.make_async_copy(source, target, small_sems.at[i])
        for i, (source, target) in enumerate(
            [
                (lens_hbm, lens_ref), (owner_hbm, owner_ref), (slot_hbm, slot_ref),
                (q_hbm, q_ref), (nk_hbm, nk_ref), (nv_hbm, nv_ref),
            ]
        )
    ]
    for c in range(steps):
        part = pl.ds(c * CHUNK, CHUNK)
        copies.append((
            pltpu.make_async_copy(k_hbm.at[part], k_buf.at[part], sems.at[0, c]),
            pltpu.make_async_copy(v_hbm.at[part], v_buf.at[part], sems.at[1, c]),
        ))
    order = [copies[c][kind] for kind in range(2) for c in range(steps)]
    for copy in small:
        copy.start()
    order[0].start()
    for copy in small:
        copy.wait()
    for copy in order[1:]:
        copy.start()

    me = position()
    row = iota((requests, 128), 0)
    lens = jnp.zeros((requests, 128), jnp.int32)
    for r in range(requests):
        lens = jnp.where(row == r, lens_ref[r], lens)
    lens = jnp.concatenate([lens] * (max_pages // 128), axis=1)
    live = jnp.clip(lens - page * iota(lens.shape, 1), 0, page)
    val = jnp.where(owner_ref[...] == me, iota(lens.shape, 0) * page + live, 0)
    hi_ref[...] = slot_ref[...] >> 5
    lo_ref[...] = slot_ref[...] & 31
    val_ref[...] = val.astype(f32)
    side = iota((SIDE, ENTRIES), 0)
    wide = BLOCK * SIDE
    table = jnp.zeros((wide, wide), f32)
    for j in range(max_pages // ENTRIES):
        lanes = slice(j * ENTRIES, (j + 1) * ENTRIES)
        for g in range(requests // BLOCK):
            put, at = [], []
            for r in range(g * BLOCK, (g + 1) * BLOCK):
                put.append(jnp.where(hi_ref[r : r + 1, lanes] == side, val_ref[r : r + 1, lanes], 0.0))
                at.append(jnp.where(lo_ref[r : r + 1, lanes] == side, 1.0, 0.0))
            table += dot_t(
                jnp.concatenate(put, axis=0).astype(bf16), jnp.concatenate(at, axis=0).astype(bf16)
            )
    same = iota((wide, wide), 0) // SIDE == iota((wide, wide), 1) // SIDE
    table = jnp.where(same, table, 0.0).astype(bf16)
    span = SIDE * page
    spread = jnp.where(
        iota((wide, span), 0) % SIDE == iota((wide, span), 1) // page, 1.0, 0.0
    ).astype(bf16)
    found = dot(table, spread)
    code = found[:SIDE]
    for b in range(1, BLOCK):
        code = code + found[b * SIDE : (b + 1) * SIDE]
    code = code.astype(jnp.int32) - 1
    key_ref[...] = jnp.where(iota(code.shape, 1) % page <= (code & (page - 1)), code >> 4, -1)

    q = q_ref[...]
    scale = math.log2(math.e) / math.sqrt(dim)
    wanted = iota((requests, span), 0)
    highest = jnp.full((rows, 128), lowest, f32)
    for c in range(steps):
        copies[c][0].wait()
        for i in range(c * CHUNK // span, (c + 1) * CHUNK // span):
            here = slice(i * span, (i + 1) * span)
            bias = jnp.where(key_ref[i : i + 1, :] == wanted, 0.0, masked)
            s = dot_t(q, k_buf[here, :]) * scale + jnp.concatenate([bias] * heads, axis=0)
            s_buf[:, here] = s
            for j in range(span // 128):
                highest = jnp.maximum(highest, s[:, j * 128 : (j + 1) * 128])
    top = jnp.max(highest, axis=1, keepdims=True)
    total = jnp.zeros((rows, 128), f32)
    out = jnp.zeros((rows, dim), f32)
    for c in range(steps):
        copies[c][1].wait()
        for i in range(c * CHUNK // STRIDE, (c + 1) * CHUNK // STRIDE):
            here = slice(i * STRIDE, (i + 1) * STRIDE)
            p = jnp.exp2(s_buf[:, here] - top)
            for j in range(STRIDE // 128):
                total = total + p[:, j * 128 : (j + 1) * 128]
            out = out + dot(p.astype(bf16), v_buf[here, :])
    total = jnp.sum(total, axis=1, keepdims=True)

    nk = jnp.concatenate([nk_ref[...].astype(f32)] * heads, axis=0)
    nv = jnp.concatenate([nv_ref[...].astype(f32)] * heads, axis=0)
    self_score = jnp.sum(q.astype(f32) * nk, axis=1, keepdims=True)
    self_score = jnp.where(me == 0, self_score * scale, masked)
    new_top = jnp.maximum(top, self_score)
    keep = jnp.exp2(top - new_top)
    take = jnp.exp2(self_score - new_top)
    out = out * keep + take * nv
    total = total * keep + take

    lane = iota((rows, 128), 1)
    group = (iota((rows, 128), 0) // requests) % 3
    meta = jnp.zeros((rows, 128), f32)
    for i, part in enumerate(split3(new_top) + split3(total)):
        meta = jnp.where(lane == 6 * group + i, part, meta)
    both = jnp.concatenate([out.astype(bf16), meta.astype(bf16)], axis=0)
    sent = out_ref.shape[0]
    to = iota((sent, 2 * rows), 0)
    source = iota((sent, 2 * rows), 1)
    inner = jnp.where(source < rows, source, source - rows)
    flat = (inner % requests) * heads + inner // requests
    data = (source < rows) & (to % 4 < 3) & (flat == (to // 4) * 3 + to % 4)
    head_row = (source >= rows) & (to % 4 == 3) & (flat // 3 == to // 4)
    pick = jnp.where(data, 1.0, jnp.where(head_row, 1.0, 0.0)).astype(bf16)
    out_ref[...] = dot(pick, both).astype(bf16)


def near_kernel(got_ref, out_ref):
    sent = got_ref.shape[0]
    blocks = sent // (4 * NEAR)
    mine = 3 * blocks
    kept = mine + 8
    got = got_ref[...]
    height = 2 * NEAR * kept
    to = iota((height, sent), 0)
    source = iota((height, sent), 1)
    line = to % kept
    near = (to // kept) % NEAR
    base = (line // 3) * (4 * NEAR) + near * 4
    wanted = jnp.where(to < NEAR * kept, base + line % 3, base + 3)
    pick = jnp.where((source == wanted) & (line < mine), 1.0, 0.0).astype(bf16)
    all_rows = dot(pick, got)
    lane = iota((kept, 128), 1)
    line = iota((kept, 128), 0)
    first = 6 * (line % 3)
    outs, tops, totals = [], [], []
    for b in range(NEAR):
        outs.append(all_rows[b * kept : (b + 1) * kept])
        meta = all_rows[(NEAR + b) * kept : (NEAR + b + 1) * kept]
        is_top = (lane >= first) & (lane < first + 3)
        is_total = (lane >= first + 3) & (lane < first + 6)
        tops.append(jnp.sum(jnp.where(is_top, meta, 0.0), axis=1, keepdims=True))
        totals.append(jnp.sum(jnp.where(is_total, meta, 0.0), axis=1, keepdims=True))
    top = tops[0]
    for t in tops[1:]:
        top = jnp.maximum(top, t)
    out = jnp.zeros((kept, 128), f32)
    total = jnp.zeros((kept, 1), f32)
    for b in range(NEAR):
        factor = jnp.exp2(tops[b] - top)
        out = out + factor * outs[b]
        total = total + factor * totals[b]
    meta = jnp.zeros((kept, 128), f32)
    for i, part in enumerate(split3(top) + split3(total)[:2]):
        meta = jnp.where((lane == line + i * mine) & (line < mine), part, meta)
    out = jnp.where(line == mine, jnp.sum(meta, axis=0, keepdims=True), out)
    block = mine + 2
    out = out.astype(bf16)[:block]
    for d in range(out_ref.shape[0] // block):
        out_ref[d * block : (d + 1) * block, :] = out


def project_kernel(got_ref, w_ref, out_ref, flat_ref, *, block):
    total_rows, dim = got_ref.shape
    far = total_rows // block // NEAR
    mine = block - 2
    flat_ref[...] = jnp.zeros(flat_ref.shape, f32)
    lane = iota((mine, 128), 1)
    line = iota((mine, 128), 0)
    is_top = (lane % mine == line) & (lane < 3 * mine)
    is_total = (lane % mine == line) & (lane >= 3 * mine) & (lane < 5 * mine)
    for b in range(NEAR):
        outs, tops, totals = [], [], []
        for a in range(far):
            first = (a * NEAR + b) * block
            x = got_ref[first : first + block, :].astype(f32)
            head = x[mine : mine + 1]
            outs.append(x[:mine])
            tops.append(jnp.sum(jnp.where(is_top, head, 0.0), axis=1, keepdims=True))
            totals.append(jnp.sum(jnp.where(is_total, head, 0.0), axis=1, keepdims=True))
        top = tops[0]
        for t in tops[1:]:
            top = jnp.maximum(top, t)
        out = jnp.zeros((mine, dim), f32)
        total = jnp.zeros((mine, 1), f32)
        for a in range(far):
            factor = jnp.exp2(tops[a] - top)
            out = out + factor * outs[a]
            total = total + factor * totals[a]
        attended = out / total
        halves = NEAR // 2
        request, half = b // halves, b % halves
        for i in range(mine):
            at = ((i // 3) * 3 * halves + half * 3 + i % 3) * dim
            flat_ref[request : request + 1, at : at + dim] = attended[i : i + 1]
    projected = dot(flat_ref[...].astype(bf16), w_ref[...])
    out_ref[...] = projected[: out_ref.shape[0]].astype(bf16)


VMEM = pl.BlockSpec(memory_space=pltpu.VMEM)
ANY = pl.BlockSpec(memory_space=pl.ANY)


def local(
    queries, k_cache, v_cache, new_key, new_value, ctx_lens, page_owner, page_slot, out_weight,
    interpret=False,
):
    _, slots, page, dim = k_cache.shape
    requests, heads, _ = queries.shape
    tokens = slots * page
    rows = requests * heads
    sent = rows // 3 * 4
    partial = attend_call(
        lambda: lax.axis_index(("far", "near")), ctx_lens, page_owner, page_slot, queries.transpose(1, 0, 2).reshape(rows, dim), new_key[0], new_value[0],
        k_cache.reshape(tokens, dim), v_cache.reshape(tokens, dim), sent, interpret,
    )
    partial, out_weight = lax.optimization_barrier((partial, out_weight))
    got = lax.all_to_all(partial, ("heads", "near"), 0, 0, tiled=True)
    peers = lax.axis_size("far") * lax.axis_size("near")
    merged = near_call(got, peers, interpret)
    block = merged.shape[0] // peers
    merged = merged.reshape(peers, block // 2, 2, dim)
    everything = lax.all_to_all(merged, ("far", "near"), 0, 0, tiled=True)
    everything = everything.reshape(peers * block, dim)
    mine = requests // lax.axis_size("heads")
    return project_call(everything, out_weight, mine, block, interpret)


def in_hbm(x):
    return pltpu.with_memory_space_constraint(x, pltpu.HBM)


def attend_call(position, lens, owner, slot, q, nk, nv, k, v, sent, interpret):
    tokens, dim = k.shape
    requests, max_pages = owner.shape
    return pl.pallas_call(
        lambda *refs: attend_kernel(*refs, position=position),
        out_shape=jax.ShapeDtypeStruct((sent, dim), bf16),
        in_specs=[ANY] * 8,
        out_specs=VMEM,
        scratch_shapes=[
            pltpu.SMEM(lens.shape, lens.dtype),
            *(pltpu.VMEM(x.shape, x.dtype) for x in (owner, slot, q, nk, nv)),
            pltpu.VMEM((tokens, dim), bf16),
            pltpu.VMEM((tokens, dim), bf16),
            pltpu.VMEM((q.shape[0], tokens), f32),
            pltpu.VMEM((requests, max_pages), jnp.int32),
            pltpu.VMEM((requests, max_pages), jnp.int32),
            pltpu.VMEM((requests, max_pages), f32),
            pltpu.VMEM((SIDE, tokens // SIDE), jnp.int32),
            pltpu.SemaphoreType.DMA((6,)),
            pltpu.SemaphoreType.DMA((2, tokens // CHUNK)),
        ],
        compiler_params=pltpu.CompilerParams(vmem_limit_bytes=24 << 20),
        interpret=interpret,
        name="attend",
    )(*(in_hbm(x) for x in (lens, owner, slot, q, nk, nv, k, v)))


def near_call(got, peers, interpret):
    sent, dim = got.shape
    block = sent // (4 * NEAR) * 3 + 2
    return pl.pallas_call(
        near_kernel,
        out_shape=jax.ShapeDtypeStruct((peers * block, dim), bf16),
        in_specs=[VMEM],
        out_specs=VMEM,
        compiler_params=pltpu.CompilerParams(vmem_limit_bytes=4 << 20),
        interpret=interpret,
        name="near",
    )(got)


def project_call(everything, w, mine, block, interpret):
    inner, features = w.shape
    return pl.pallas_call(
        lambda *refs: project_kernel(*refs, block=block),
        out_shape=jax.ShapeDtypeStruct((mine, features), bf16),
        in_specs=[VMEM, VMEM],
        out_specs=VMEM,
        scratch_shapes=[pltpu.VMEM((8, inner), f32)],
        compiler_params=pltpu.CompilerParams(vmem_limit_bytes=8 << 20),
        interpret=interpret,
        name="project",
    )(everything, pltpu.with_memory_space_constraint(w, pltpu.VMEM))


def solution(mesh):
    torus = Mesh(
        mesh.devices.reshape(
            mesh.shape["group"], mesh.shape["pages"] // NEAR, NEAR, mesh.shape["heads"]
        ),
        ("group", "far", "near", "heads"),
    )
    pages = ("far", "near")
    in_specs = (
        P("group", "heads", None),
        P("heads", ("group", *pages), None, None),
        P("heads", ("group", *pages), None, None),
        P("heads", "group", None),
        P("heads", "group", None),
        P("group"),
        P("group", None),
        P("group", None),
        P(None, pages),
    )
    out_specs = P(("group", "heads"), pages)
    return jax.shard_map(local, mesh=torus, in_specs=in_specs, out_specs=out_specs, check_vma=False)
```

```python
import math

import jax
import jax.numpy as jnp
from jax import lax
from jax.experimental import pallas as pl
from jax.experimental.pallas import tpu as pltpu
from jax.sharding import Mesh
from jax.sharding import PartitionSpec as P

NEAR = 4
CHUNK = 8192
STRIDE = 1024
SIDE = 32
BLOCK = 4
ENTRIES = 256

f32 = jnp.float32
bf16 = jnp.bfloat16
masked = -1e30
lowest = -1e29


def iota(shape, dim):
    return lax.broadcasted_iota(jnp.int32, shape, dim)


def dot(a, b):
    return jnp.dot(a, b, preferred_element_type=f32)


def dot_t(a, b):
    return lax.dot_general(a, b, (((1,), (1,)), ((), ())), preferred_element_type=f32)


def split3(x):
    hi = x.astype(bf16).astype(f32)
    mid = (x - hi).astype(bf16).astype(f32)
    lo = (x - hi - mid).astype(bf16).astype(f32)
    return [hi, mid, lo]


def attend_kernel(
    lens_hbm, owner_hbm, slot_hbm, q_hbm, nk_hbm, nv_hbm, k_hbm, v_hbm, out_ref,
    lens_ref, owner_ref, slot_ref, q_ref, nk_ref, nv_ref,
    k_buf, v_buf, s_buf, hi_ref, lo_ref, val_ref, key_ref, small_sems, sems, *, position,
):
    requests, max_pages = owner_ref.shape
    rows, dim = q_ref.shape
    heads = rows // requests
    tokens = k_buf.shape[0]
    page = tokens // (SIDE * SIDE)
    steps = tokens // CHUNK
    copies = []
    small = [
        pltpu.make_async_copy(source, target, small_sems.at[i])
        for i, (source, target) in enumerate(
            [
                (lens_hbm, lens_ref), (owner_hbm, owner_ref), (slot_hbm, slot_ref),
                (q_hbm, q_ref), (nk_hbm, nk_ref), (nv_hbm, nv_ref),
            ]
        )
    ]
    for c in range(steps):
        part = pl.ds(c * CHUNK, CHUNK)
        copies.append((
            pltpu.make_async_copy(k_hbm.at[part], k_buf.at[part], sems.at[0, c]),
            pltpu.make_async_copy(v_hbm.at[part], v_buf.at[part], sems.at[1, c]),
        ))
    order = [copies[c][kind] for kind in range(2) for c in range(steps)]
    for copy in small:
        copy.start()
    order[0].start()
    for copy in small:
        copy.wait()
    for copy in order[1:]:
        copy.start()

    me = position()
    row = iota((requests, 128), 0)
    lens = jnp.zeros((requests, 128), jnp.int32)
    for r in range(requests):
        lens = jnp.where(row == r, lens_ref[r], lens)
    lens = jnp.concatenate([lens] * (max_pages // 128), axis=1)
    live = jnp.clip(lens - page * iota(lens.shape, 1), 0, page)
    val = jnp.where(owner_ref[...] == me, iota(lens.shape, 0) * page + live, 0)
    hi_ref[...] = slot_ref[...] >> 5
    lo_ref[...] = slot_ref[...] & 31
    val_ref[...] = val.astype(f32)
    side = iota((SIDE, ENTRIES), 0)
    wide = BLOCK * SIDE
    table = jnp.zeros((wide, wide), f32)
    for j in range(max_pages // ENTRIES):
        lanes = slice(j * ENTRIES, (j + 1) * ENTRIES)
        for g in range(requests // BLOCK):
            put, at = [], []
            for r in range(g * BLOCK, (g + 1) * BLOCK):
                put.append(jnp.where(hi_ref[r : r + 1, lanes] == side, val_ref[r : r + 1, lanes], 0.0))
                at.append(jnp.where(lo_ref[r : r + 1, lanes] == side, 1.0, 0.0))
            table += dot_t(
                jnp.concatenate(put, axis=0).astype(bf16), jnp.concatenate(at, axis=0).astype(bf16)
            )
    same = iota((wide, wide), 0) // SIDE == iota((wide, wide), 1) // SIDE
    table = jnp.where(same, table, 0.0).astype(bf16)
    span = SIDE * page
    spread = jnp.where(
        iota((wide, span), 0) % SIDE == iota((wide, span), 1) // page, 1.0, 0.0
    ).astype(bf16)
    found = dot(table, spread)
    code = found[:SIDE]
    for b in range(1, BLOCK):
        code = code + found[b * SIDE : (b + 1) * SIDE]
    code = code.astype(jnp.int32) - 1
    key_ref[...] = jnp.where(iota(code.shape, 1) % page <= (code & (page - 1)), code >> 4, -1)

    q = q_ref[...]
    scale = math.log2(math.e) / math.sqrt(dim)
    wanted = iota((requests, span), 0)
    highest = jnp.full((rows, 128), lowest, f32)
    for c in range(steps):
        copies[c][0].wait()
        for i in range(c * CHUNK // span, (c + 1) * CHUNK // span):
            here = slice(i * span, (i + 1) * span)
            bias = jnp.where(key_ref[i : i + 1, :] == wanted, 0.0, masked)
            s = dot_t(q, k_buf[here, :]) * scale + jnp.concatenate([bias] * heads, axis=0)
            s_buf[:, here] = s
            for j in range(span // 128):
                highest = jnp.maximum(highest, s[:, j * 128 : (j + 1) * 128])
    top = jnp.max(highest, axis=1, keepdims=True)
    total = jnp.zeros((rows, 128), f32)
    out = jnp.zeros((rows, dim), f32)
    for c in range(steps):
        copies[c][1].wait()
        for i in range(c * CHUNK // STRIDE, (c + 1) * CHUNK // STRIDE):
            here = slice(i * STRIDE, (i + 1) * STRIDE)
            p = jnp.exp2(s_buf[:, here] - top)
            for j in range(STRIDE // 128):
                total = total + p[:, j * 128 : (j + 1) * 128]
            out = out + dot(p.astype(bf16), v_buf[here, :])
    total = jnp.sum(total, axis=1, keepdims=True)

    nk = jnp.concatenate([nk_ref[...].astype(f32)] * heads, axis=0)
    nv = jnp.concatenate([nv_ref[...].astype(f32)] * heads, axis=0)
    self_score = jnp.sum(q.astype(f32) * nk, axis=1, keepdims=True)
    self_score = jnp.where(me == 0, self_score * scale, masked)
    new_top = jnp.maximum(top, self_score)
    keep = jnp.exp2(top - new_top)
    take = jnp.exp2(self_score - new_top)
    out = out * keep + take * nv
    total = total * keep + take

    lane = iota((rows, 128), 1)
    group = (iota((rows, 128), 0) // requests) % 3
    meta = jnp.zeros((rows, 128), f32)
    for i, part in enumerate(split3(new_top) + split3(total)):
        meta = jnp.where(lane == 6 * group + i, part, meta)
    both = jnp.concatenate([out.astype(bf16), meta.astype(bf16)], axis=0)
    sent = out_ref.shape[0]
    to = iota((sent, 2 * rows), 0)
    source = iota((sent, 2 * rows), 1)
    inner = jnp.where(source < rows, source, source - rows)
    flat = (inner % requests) * heads + inner // requests
    data = (source < rows) & (to % 4 < 3) & (flat == (to // 4) * 3 + to % 4)
    head_row = (source >= rows) & (to % 4 == 3) & (flat // 3 == to // 4)
    pick = jnp.where(data, 1.0, jnp.where(head_row, 1.0, 0.0)).astype(bf16)
    out_ref[...] = dot(pick, both).astype(bf16)


def near_kernel(got_ref, out_ref):
    sent = got_ref.shape[0]
    blocks = sent // (4 * NEAR)
    mine = 3 * blocks
    kept = mine + 8
    got = got_ref[...]
    height = 2 * NEAR * kept
    to = iota((height, sent), 0)
    source = iota((height, sent), 1)
    line = to % kept
    near = (to // kept) % NEAR
    base = (line // 3) * (4 * NEAR) + near * 4
    wanted = jnp.where(to < NEAR * kept, base + line % 3, base + 3)
    pick = jnp.where((source == wanted) & (line < mine), 1.0, 0.0).astype(bf16)
    all_rows = dot(pick, got)
    lane = iota((kept, 128), 1)
    line = iota((kept, 128), 0)
    first = 6 * (line % 3)
    outs, tops, totals = [], [], []
    for b in range(NEAR):
        outs.append(all_rows[b * kept : (b + 1) * kept])
        meta = all_rows[(NEAR + b) * kept : (NEAR + b + 1) * kept]
        is_top = (lane >= first) & (lane < first + 3)
        is_total = (lane >= first + 3) & (lane < first + 6)
        tops.append(jnp.sum(jnp.where(is_top, meta, 0.0), axis=1, keepdims=True))
        totals.append(jnp.sum(jnp.where(is_total, meta, 0.0), axis=1, keepdims=True))
    top = tops[0]
    for t in tops[1:]:
        top = jnp.maximum(top, t)
    out = jnp.zeros((kept, 128), f32)
    total = jnp.zeros((kept, 1), f32)
    for b in range(NEAR):
        factor = jnp.exp2(tops[b] - top)
        out = out + factor * outs[b]
        total = total + factor * totals[b]
    meta = jnp.zeros((kept, 128), f32)
    for i, part in enumerate(split3(top) + split3(total)[:2]):
        meta = jnp.where((lane == line + i * mine) & (line < mine), part, meta)
    out = jnp.where(line == mine, jnp.sum(meta, axis=0, keepdims=True), out)
    block = mine + 2
    out = out.astype(bf16)[:block]
    for d in range(out_ref.shape[0] // block):
        out_ref[d * block : (d + 1) * block, :] = out


def project_kernel(got_ref, w_ref, out_ref, flat_ref, *, block):
    total_rows, dim = got_ref.shape
    far = total_rows // block // NEAR
    mine = block - 2
    flat_ref[...] = jnp.zeros(flat_ref.shape, f32)
    lane = iota((mine, 128), 1)
    line = iota((mine, 128), 0)
    is_top = (lane % mine == line) & (lane < 3 * mine)
    is_total = (lane % mine == line) & (lane >= 3 * mine) & (lane < 5 * mine)
    for b in range(NEAR):
        outs, tops, totals = [], [], []
        for a in range(far):
            first = (a * NEAR + b) * block
            x = got_ref[first : first + block, :].astype(f32)
            head = x[mine : mine + 1]
            outs.append(x[:mine])
            tops.append(jnp.sum(jnp.where(is_top, head, 0.0), axis=1, keepdims=True))
            totals.append(jnp.sum(jnp.where(is_total, head, 0.0), axis=1, keepdims=True))
        top = tops[0]
        for t in tops[1:]:
            top = jnp.maximum(top, t)
        out = jnp.zeros((mine, dim), f32)
        total = jnp.zeros((mine, 1), f32)
        for a in range(far):
            factor = jnp.exp2(tops[a] - top)
            out = out + factor * outs[a]
            total = total + factor * totals[a]
        attended = out / total
        halves = NEAR // 2
        request, half = b // halves, b % halves
        for i in range(mine):
            at = ((i // 3) * 3 * halves + half * 3 + i % 3) * dim
            flat_ref[request : request + 1, at : at + dim] = attended[i : i + 1]
    projected = dot(flat_ref[...].astype(bf16), w_ref[...])
    out_ref[...] = projected[: out_ref.shape[0]].astype(bf16)


VMEM = pl.BlockSpec(memory_space=pltpu.VMEM)
ANY = pl.BlockSpec(memory_space=pl.ANY)


def local(
    queries, k_cache, v_cache, new_key, new_value, ctx_lens, page_owner, page_slot, out_weight,
    interpret=False,
):
    _, slots, page, dim = k_cache.shape
    requests, heads, _ = queries.shape
    tokens = slots * page
    rows = requests * heads
    sent = rows // 3 * 4
    partial = attend_call(
        lambda: lax.axis_index(("far", "near")), ctx_lens, page_owner, page_slot, queries.transpose(1, 0, 2).reshape(rows, dim), new_key[0], new_value[0],
        k_cache.reshape(tokens, dim), v_cache.reshape(tokens, dim), sent, interpret,
    )
    partial, out_weight = lax.optimization_barrier((partial, out_weight))
    got = lax.all_to_all(partial, ("heads", "near"), 0, 0, tiled=True)
    peers = lax.axis_size("far") * lax.axis_size("near")
    merged = near_call(got, peers, interpret)
    block = merged.shape[0] // peers
    merged = merged.reshape(peers, block // 2, 2, dim)
    everything = lax.all_to_all(merged, ("far", "near"), 0, 0, tiled=True)
    everything = everything.reshape(peers * block, dim)
    mine = requests // lax.axis_size("heads")
    return project_call(everything, out_weight, mine, block, interpret)


def in_hbm(x):
    return pltpu.with_memory_space_constraint(x, pltpu.HBM)


def attend_call(position, lens, owner, slot, q, nk, nv, k, v, sent, interpret):
    tokens, dim = k.shape
    requests, max_pages = owner.shape
    return pl.pallas_call(
        lambda *refs: attend_kernel(*refs, position=position),
        out_shape=jax.ShapeDtypeStruct((sent, dim), bf16),
        in_specs=[ANY] * 8,
        out_specs=VMEM,
        scratch_shapes=[
            pltpu.SMEM(lens.shape, lens.dtype),
            *(pltpu.VMEM(x.shape, x.dtype) for x in (owner, slot, q, nk, nv)),
            pltpu.VMEM((tokens, dim), bf16),
            pltpu.VMEM((tokens, dim), bf16),
            pltpu.VMEM((q.shape[0], tokens), f32),
            pltpu.VMEM((requests, max_pages), jnp.int32),
            pltpu.VMEM((requests, max_pages), jnp.int32),
            pltpu.VMEM((requests, max_pages), f32),
            pltpu.VMEM((SIDE, tokens // SIDE), jnp.int32),
            pltpu.SemaphoreType.DMA((6,)),
            pltpu.SemaphoreType.DMA((2, tokens // CHUNK)),
        ],
        compiler_params=pltpu.CompilerParams(vmem_limit_bytes=24 << 20),
        interpret=interpret,
        name="attend",
    )(*(in_hbm(x) for x in (lens, owner, slot, q, nk, nv, k, v)))


def near_call(got, peers, interpret):
    sent, dim = got.shape
    block = sent // (4 * NEAR) * 3 + 2
    return pl.pallas_call(
        near_kernel,
        out_shape=jax.ShapeDtypeStruct((peers * block, dim), bf16),
        in_specs=[VMEM],
        out_specs=VMEM,
        compiler_params=pltpu.CompilerParams(vmem_limit_bytes=4 << 20),
        cost_estimate=pl.CostEstimate(flops=10**13, transcendentals=0, bytes_accessed=0),
        interpret=interpret,
        name="near",
    )(got)


def project_call(everything, w, mine, block, interpret):
    inner, features = w.shape
    return pl.pallas_call(
        lambda *refs: project_kernel(*refs, block=block),
        out_shape=jax.ShapeDtypeStruct((mine, features), bf16),
        in_specs=[VMEM, VMEM],
        out_specs=VMEM,
        scratch_shapes=[pltpu.VMEM((8, inner), f32)],
        compiler_params=pltpu.CompilerParams(vmem_limit_bytes=8 << 20),
        interpret=interpret,
        name="project",
    )(everything, pltpu.with_memory_space_constraint(w, pltpu.VMEM))


def solution(mesh):
    torus = Mesh(
        mesh.devices.reshape(
            mesh.shape["group"], mesh.shape["pages"] // NEAR, NEAR, mesh.shape["heads"]
        ),
        ("group", "far", "near", "heads"),
    )
    pages = ("far", "near")
    in_specs = (
        P("group", "heads", None),
        P("heads", ("group", *pages), None, None),
        P("heads", ("group", *pages), None, None),
        P("heads", "group", None),
        P("heads", "group", None),
        P("group"),
        P("group", None),
        P("group", None),
        P(None, pages),
    )
    out_specs = P(("group", "heads"), pages)
    return jax.shard_map(local, mesh=torus, in_specs=in_specs, out_specs=out_specs, check_vma=False)
```

```python
import math

import jax
import jax.numpy as jnp
from jax import lax
from jax.experimental import pallas as pl
from jax.experimental.pallas import tpu as pltpu
from jax.sharding import Mesh
from jax.sharding import PartitionSpec as P

NEAR = 4
CHUNK = 8192
STRIDE = 1024
SIDE = 32
BLOCK = 4
ENTRIES = 256

f32 = jnp.float32
bf16 = jnp.bfloat16
masked = -1e30
lowest = -1e29


def iota(shape, dim):
    return lax.broadcasted_iota(jnp.int32, shape, dim)


def dot(a, b):
    return jnp.dot(a, b, preferred_element_type=f32)


def dot_t(a, b):
    return lax.dot_general(a, b, (((1,), (1,)), ((), ())), preferred_element_type=f32)


def split3(x):
    hi = x.astype(bf16).astype(f32)
    mid = (x - hi).astype(bf16).astype(f32)
    lo = (x - hi - mid).astype(bf16).astype(f32)
    return [hi, mid, lo]


def attend_kernel(
    lens_hbm, owner_hbm, slot_hbm, q_hbm, nk_hbm, nv_hbm, k_hbm, v_hbm, out_ref,
    lens_ref, owner_ref, slot_ref, q_ref, nk_ref, nv_ref,
    k_buf, v_buf, s_buf, hi_ref, lo_ref, val_ref, key_ref, small_sems, sems, *, position,
):
    requests, max_pages = owner_ref.shape
    rows, dim = q_ref.shape
    heads = rows // requests
    tokens = k_buf.shape[0]
    page = tokens // (SIDE * SIDE)
    steps = tokens // CHUNK
    copies = []
    small = [
        pltpu.make_async_copy(source, target, small_sems.at[i])
        for i, (source, target) in enumerate(
            [
                (lens_hbm, lens_ref), (owner_hbm, owner_ref), (slot_hbm, slot_ref),
                (q_hbm, q_ref), (nk_hbm, nk_ref), (nv_hbm, nv_ref),
            ]
        )
    ]
    for c in range(steps):
        part = pl.ds(c * CHUNK, CHUNK)
        copies.append((
            pltpu.make_async_copy(k_hbm.at[part], k_buf.at[part], sems.at[0, c]),
            pltpu.make_async_copy(v_hbm.at[part], v_buf.at[part], sems.at[1, c]),
        ))
    order = [copies[c][kind] for kind in range(2) for c in range(steps)]
    for copy in small:
        copy.start()
    order[0].start()
    for copy in small:
        copy.wait()
    for copy in order[1:]:
        copy.start()

    me = position()
    row = iota((requests, 128), 0)
    lens = jnp.zeros((requests, 128), jnp.int32)
    for r in range(requests):
        lens = jnp.where(row == r, lens_ref[r], lens)
    lens = jnp.concatenate([lens] * (max_pages // 128), axis=1)
    live = jnp.clip(lens - page * iota(lens.shape, 1), 0, page)
    val = jnp.where(owner_ref[...] == me, iota(lens.shape, 0) * page + live, 0)
    hi_ref[...] = slot_ref[...] >> 5
    lo_ref[...] = slot_ref[...] & 31
    val_ref[...] = val.astype(f32)
    side = iota((SIDE, ENTRIES), 0)
    wide = BLOCK * SIDE
    table = jnp.zeros((wide, wide), f32)
    for j in range(max_pages // ENTRIES):
        lanes = slice(j * ENTRIES, (j + 1) * ENTRIES)
        for g in range(requests // BLOCK):
            put, at = [], []
            for r in range(g * BLOCK, (g + 1) * BLOCK):
                put.append(jnp.where(hi_ref[r : r + 1, lanes] == side, val_ref[r : r + 1, lanes], 0.0))
                at.append(jnp.where(lo_ref[r : r + 1, lanes] == side, 1.0, 0.0))
            table += dot_t(
                jnp.concatenate(put, axis=0).astype(bf16), jnp.concatenate(at, axis=0).astype(bf16)
            )
    same = iota((wide, wide), 0) // SIDE == iota((wide, wide), 1) // SIDE
    table = jnp.where(same, table, 0.0).astype(bf16)
    span = SIDE * page
    spread = jnp.where(
        iota((wide, span), 0) % SIDE == iota((wide, span), 1) // page, 1.0, 0.0
    ).astype(bf16)
    found = dot(table, spread)
    code = found[:SIDE]
    for b in range(1, BLOCK):
        code = code + found[b * SIDE : (b + 1) * SIDE]
    code = code.astype(jnp.int32) - 1
    key_ref[...] = jnp.where(iota(code.shape, 1) % page <= (code & (page - 1)), code >> 4, -1)

    q = q_ref[...]
    scale = math.log2(math.e) / math.sqrt(dim)
    wanted = iota((requests, span), 0)
    highest = jnp.full((rows, 128), lowest, f32)
    for c in range(steps):
        copies[c][0].wait()
        for i in range(c * CHUNK // span, (c + 1) * CHUNK // span):
            here = slice(i * span, (i + 1) * span)
            bias = jnp.where(key_ref[i : i + 1, :] == wanted, 0.0, masked)
            s = dot_t(q, k_buf[here, :]) * scale + jnp.concatenate([bias] * heads, axis=0)
            s_buf[:, here] = s
            for j in range(span // 128):
                highest = jnp.maximum(highest, s[:, j * 128 : (j + 1) * 128])
    top = jnp.max(highest, axis=1, keepdims=True)
    total = jnp.zeros((rows, 128), f32)
    out = jnp.zeros((rows, dim), f32)
    for c in range(steps):
        copies[c][1].wait()
        for i in range(c * CHUNK // STRIDE, (c + 1) * CHUNK // STRIDE):
            here = slice(i * STRIDE, (i + 1) * STRIDE)
            p = jnp.exp2(s_buf[:, here] - top)
            for j in range(STRIDE // 128):
                total = total + p[:, j * 128 : (j + 1) * 128]
            out = out + dot(p.astype(bf16), v_buf[here, :])
    total = jnp.sum(total, axis=1, keepdims=True)

    nk = jnp.concatenate([nk_ref[...].astype(f32)] * heads, axis=0)
    nv = jnp.concatenate([nv_ref[...].astype(f32)] * heads, axis=0)
    self_score = jnp.sum(q.astype(f32) * nk, axis=1, keepdims=True)
    self_score = jnp.where(me == 0, self_score * scale, masked)
    new_top = jnp.maximum(top, self_score)
    keep = jnp.exp2(top - new_top)
    take = jnp.exp2(self_score - new_top)
    out = out * keep + take * nv
    total = total * keep + take

    lane = iota((rows, 128), 1)
    group = (iota((rows, 128), 0) // requests) % 3
    meta = jnp.zeros((rows, 128), f32)
    for i, part in enumerate(split3(new_top) + split3(total)):
        meta = jnp.where(lane == 6 * group + i, part, meta)
    both = jnp.concatenate([out.astype(bf16), meta.astype(bf16)], axis=0)
    sent = out_ref.shape[0]
    to = iota((sent, 2 * rows), 0)
    source = iota((sent, 2 * rows), 1)
    inner = jnp.where(source < rows, source, source - rows)
    flat = (inner % requests) * heads + inner // requests
    peers = sent // (4 * NEAR)
    third = (to // 4) % peers * NEAR + to // 4 // peers
    data = (source < rows) & (to % 4 < 3) & (flat == third * 3 + to % 4)
    head_row = (source >= rows) & (to % 4 == 3) & (flat // 3 == third)
    pick = jnp.where(data, 1.0, jnp.where(head_row, 1.0, 0.0)).astype(bf16)
    out_ref[...] = dot(pick, both).astype(bf16)


def near_kernel(got_ref, out_ref):
    sent = got_ref.shape[0]
    blocks = sent // (4 * NEAR)
    mine = 3 * blocks
    kept = mine + 8
    got = got_ref[...]
    height = 2 * NEAR * kept
    to = iota((height, sent), 0)
    source = iota((height, sent), 1)
    line = to % kept
    near = (to // kept) % NEAR
    base = near * (4 * blocks) + (line // 3) * 4
    wanted = jnp.where(to < NEAR * kept, base + line % 3, base + 3)
    pick = jnp.where((source == wanted) & (line < mine), 1.0, 0.0).astype(bf16)
    all_rows = dot(pick, got)
    lane = iota((kept, 128), 1)
    line = iota((kept, 128), 0)
    first = 6 * (line % 3)
    outs, tops, totals = [], [], []
    for b in range(NEAR):
        outs.append(all_rows[b * kept : (b + 1) * kept])
        meta = all_rows[(NEAR + b) * kept : (NEAR + b + 1) * kept]
        is_top = (lane >= first) & (lane < first + 3)
        is_total = (lane >= first + 3) & (lane < first + 6)
        tops.append(jnp.sum(jnp.where(is_top, meta, 0.0), axis=1, keepdims=True))
        totals.append(jnp.sum(jnp.where(is_total, meta, 0.0), axis=1, keepdims=True))
    top = tops[0]
    for t in tops[1:]:
        top = jnp.maximum(top, t)
    out = jnp.zeros((kept, 128), f32)
    total = jnp.zeros((kept, 1), f32)
    for b in range(NEAR):
        factor = jnp.exp2(tops[b] - top)
        out = out + factor * outs[b]
        total = total + factor * totals[b]
    meta = jnp.zeros((kept, 128), f32)
    for i, part in enumerate(split3(top) + split3(total)[:2]):
        meta = jnp.where((lane == line + i * mine) & (line < mine), part, meta)
    out = jnp.where(line == mine, jnp.sum(meta, axis=0, keepdims=True), out)
    block = mine + 2
    out = out.astype(bf16)[:block]
    for d in range(out_ref.shape[0] // block):
        out_ref[d * block : (d + 1) * block, :] = out


def project_kernel(got_ref, w_ref, out_ref, flat_ref, *, block):
    total_rows, dim = got_ref.shape
    far = total_rows // block // NEAR
    mine = block - 2
    flat_ref[...] = jnp.zeros(flat_ref.shape, f32)
    lane = iota((mine, 128), 1)
    line = iota((mine, 128), 0)
    is_top = (lane % mine == line) & (lane < 3 * mine)
    is_total = (lane % mine == line) & (lane >= 3 * mine) & (lane < 5 * mine)
    for b in range(NEAR):
        outs, tops, totals = [], [], []
        for a in range(far):
            first = (a * NEAR + b) * block
            x = got_ref[first : first + block, :].astype(f32)
            head = x[mine : mine + 1]
            outs.append(x[:mine])
            tops.append(jnp.sum(jnp.where(is_top, head, 0.0), axis=1, keepdims=True))
            totals.append(jnp.sum(jnp.where(is_total, head, 0.0), axis=1, keepdims=True))
        top = tops[0]
        for t in tops[1:]:
            top = jnp.maximum(top, t)
        out = jnp.zeros((mine, dim), f32)
        total = jnp.zeros((mine, 1), f32)
        for a in range(far):
            factor = jnp.exp2(tops[a] - top)
            out = out + factor * outs[a]
            total = total + factor * totals[a]
        attended = out / total
        halves = NEAR // 2
        request, half = b // halves, b % halves
        for i in range(mine):
            at = ((i // 3) * 3 * halves + half * 3 + i % 3) * dim
            flat_ref[request : request + 1, at : at + dim] = attended[i : i + 1]
    projected = dot(flat_ref[...].astype(bf16), w_ref[...])
    out_ref[...] = projected[: out_ref.shape[0]].astype(bf16)


VMEM = pl.BlockSpec(memory_space=pltpu.VMEM)
ANY = pl.BlockSpec(memory_space=pl.ANY)


def local(
    queries, k_cache, v_cache, new_key, new_value, ctx_lens, page_owner, page_slot, out_weight,
    interpret=False,
):
    _, slots, page, dim = k_cache.shape
    requests, heads, _ = queries.shape
    tokens = slots * page
    rows = requests * heads
    sent = rows // 3 * 4
    partial = attend_call(
        lambda: lax.axis_index(("far", "near")), ctx_lens, page_owner, page_slot, queries.transpose(1, 0, 2).reshape(rows, dim), new_key[0], new_value[0],
        k_cache.reshape(tokens, dim), v_cache.reshape(tokens, dim), sent, interpret,
    )
    partial, out_weight = lax.optimization_barrier((partial, out_weight))
    got = lax.all_to_all(partial, ("near", "heads"), 0, 0, tiled=True)
    peers = lax.axis_size("far") * lax.axis_size("near")
    merged = near_call(got, peers, interpret)
    block = merged.shape[0] // peers
    merged = merged.reshape(peers, block // 2, 2, dim)
    everything = lax.all_to_all(merged, ("far", "near"), 0, 0, tiled=True)
    everything = everything.reshape(peers * block, dim)
    mine = requests // lax.axis_size("heads")
    return project_call(everything, out_weight, mine, block, interpret)


def in_hbm(x):
    return pltpu.with_memory_space_constraint(x, pltpu.HBM)


def attend_call(position, lens, owner, slot, q, nk, nv, k, v, sent, interpret):
    tokens, dim = k.shape
    requests, max_pages = owner.shape
    return pl.pallas_call(
        lambda *refs: attend_kernel(*refs, position=position),
        out_shape=jax.ShapeDtypeStruct((sent, dim), bf16),
        in_specs=[ANY] * 8,
        out_specs=VMEM,
        scratch_shapes=[
            pltpu.SMEM(lens.shape, lens.dtype),
            *(pltpu.VMEM(x.shape, x.dtype) for x in (owner, slot, q, nk, nv)),
            pltpu.VMEM((tokens, dim), bf16),
            pltpu.VMEM((tokens, dim), bf16),
            pltpu.VMEM((q.shape[0], tokens), f32),
            pltpu.VMEM((requests, max_pages), jnp.int32),
            pltpu.VMEM((requests, max_pages), jnp.int32),
            pltpu.VMEM((requests, max_pages), f32),
            pltpu.VMEM((SIDE, tokens // SIDE), jnp.int32),
            pltpu.SemaphoreType.DMA((6,)),
            pltpu.SemaphoreType.DMA((2, tokens // CHUNK)),
        ],
        compiler_params=pltpu.CompilerParams(vmem_limit_bytes=24 << 20),
        interpret=interpret,
        name="attend",
    )(*(in_hbm(x) for x in (lens, owner, slot, q, nk, nv, k, v)))


def near_call(got, peers, interpret):
    sent, dim = got.shape
    block = sent // (4 * NEAR) * 3 + 2
    return pl.pallas_call(
        near_kernel,
        out_shape=jax.ShapeDtypeStruct((peers * block, dim), bf16),
        in_specs=[VMEM],
        out_specs=VMEM,
        compiler_params=pltpu.CompilerParams(vmem_limit_bytes=4 << 20),
        interpret=interpret,
        name="near",
    )(got)


def project_call(everything, w, mine, block, interpret):
    inner, features = w.shape
    return pl.pallas_call(
        lambda *refs: project_kernel(*refs, block=block),
        out_shape=jax.ShapeDtypeStruct((mine, features), bf16),
        in_specs=[VMEM, VMEM],
        out_specs=VMEM,
        scratch_shapes=[pltpu.VMEM((8, inner), f32)],
        compiler_params=pltpu.CompilerParams(vmem_limit_bytes=8 << 20),
        interpret=interpret,
        name="project",
    )(everything, pltpu.with_memory_space_constraint(w, pltpu.VMEM))


def solution(mesh):
    torus = Mesh(
        mesh.devices.reshape(
            mesh.shape["group"], mesh.shape["pages"] // NEAR, NEAR, mesh.shape["heads"]
        ),
        ("group", "far", "near", "heads"),
    )
    pages = ("far", "near")
    in_specs = (
        P("group", "heads", None),
        P("heads", ("group", *pages), None, None),
        P("heads", ("group", *pages), None, None),
        P("heads", "group", None),
        P("heads", "group", None),
        P("group"),
        P("group", None),
        P("group", None),
        P(None, pages),
    )
    out_specs = P(("group", "heads"), pages)
    return jax.shard_map(local, mesh=torus, in_specs=in_specs, out_specs=out_specs, check_vma=False)
```

```python
import math

import jax
import jax.numpy as jnp
from jax import lax
from jax.experimental import pallas as pl
from jax.experimental.pallas import tpu as pltpu
from jax.sharding import Mesh
from jax.sharding import PartitionSpec as P

NEAR = 4
CHUNK = 8192
STRIDE = 1024
SIDE = 32
BLOCK = 4
ENTRIES = 256

f32 = jnp.float32
bf16 = jnp.bfloat16
masked = -1e30
lowest = -1e29


def iota(shape, dim):
    return lax.broadcasted_iota(jnp.int32, shape, dim)


def dot(a, b):
    return jnp.dot(a, b, preferred_element_type=f32)


def dot_t(a, b):
    return lax.dot_general(a, b, (((1,), (1,)), ((), ())), preferred_element_type=f32)


def split3(x):
    hi = x.astype(bf16).astype(f32)
    mid = (x - hi).astype(bf16).astype(f32)
    lo = (x - hi - mid).astype(bf16).astype(f32)
    return [hi, mid, lo]


def attend_kernel(
    lens_hbm, owner_hbm, slot_hbm, q_hbm, nk_hbm, nv_hbm, k_hbm, v_hbm, out_ref,
    lens_ref, owner_ref, slot_ref, q_ref, nk_ref, nv_ref,
    k_buf, v_buf, s_buf, hi_ref, lo_ref, val_ref, key_ref, small_sems, sems, *, position,
):
    requests, max_pages = owner_ref.shape
    rows, dim = q_ref.shape
    heads = rows // requests
    tokens = k_buf.shape[0]
    page = tokens // (SIDE * SIDE)
    steps = tokens // CHUNK
    copies = []
    small = [
        pltpu.make_async_copy(source, target, small_sems.at[i])
        for i, (source, target) in enumerate(
            [
                (lens_hbm, lens_ref), (owner_hbm, owner_ref), (slot_hbm, slot_ref),
                (q_hbm, q_ref), (nk_hbm, nk_ref), (nv_hbm, nv_ref),
            ]
        )
    ]
    for c in range(steps):
        part = pl.ds(c * CHUNK, CHUNK)
        copies.append((
            pltpu.make_async_copy(k_hbm.at[part], k_buf.at[part], sems.at[0, c]),
            pltpu.make_async_copy(v_hbm.at[part], v_buf.at[part], sems.at[1, c]),
        ))
    order = [copies[c][kind] for kind in range(2) for c in range(steps)]
    for copy in small:
        copy.start()
    order[0].start()
    lane = iota((rows, 128), 1)
    group = (iota((rows, 128), 0) // requests) % 3
    sent = out_ref.shape[0]
    to = iota((sent, 2 * rows), 0)
    source = iota((sent, 2 * rows), 1)
    inner = jnp.where(source < rows, source, source - rows)
    flat = (inner % requests) * heads + inner // requests
    data = (source < rows) & (to % 4 < 3) & (flat == (to // 4) * 3 + to % 4)
    head_row = (source >= rows) & (to % 4 == 3) & (flat // 3 == to // 4)
    pick = jnp.where(data, 1.0, jnp.where(head_row, 1.0, 0.0)).astype(bf16)
    for copy in small:
        copy.wait()
    for copy in order[1:]:
        copy.start()

    me = position()
    row = iota((requests, 128), 0)
    lens = jnp.zeros((requests, 128), jnp.int32)
    for r in range(requests):
        lens = jnp.where(row == r, lens_ref[r], lens)
    lens = jnp.concatenate([lens] * (max_pages // 128), axis=1)
    live = jnp.clip(lens - page * iota(lens.shape, 1), 0, page)
    val = jnp.where(owner_ref[...] == me, iota(lens.shape, 0) * page + live, 0)
    hi_ref[...] = slot_ref[...] >> 5
    lo_ref[...] = slot_ref[...] & 31
    val_ref[...] = val.astype(f32)
    side = iota((SIDE, ENTRIES), 0)
    wide = BLOCK * SIDE
    table = jnp.zeros((wide, wide), f32)
    for j in range(max_pages // ENTRIES):
        lanes = slice(j * ENTRIES, (j + 1) * ENTRIES)
        for g in range(requests // BLOCK):
            put, at = [], []
            for r in range(g * BLOCK, (g + 1) * BLOCK):
                put.append(jnp.where(hi_ref[r : r + 1, lanes] == side, val_ref[r : r + 1, lanes], 0.0))
                at.append(jnp.where(lo_ref[r : r + 1, lanes] == side, 1.0, 0.0))
            table += dot_t(
                jnp.concatenate(put, axis=0).astype(bf16), jnp.concatenate(at, axis=0).astype(bf16)
            )
    same = iota((wide, wide), 0) // SIDE == iota((wide, wide), 1) // SIDE
    table = jnp.where(same, table, 0.0).astype(bf16)
    span = SIDE * page
    spread = jnp.where(
        iota((wide, span), 0) % SIDE == iota((wide, span), 1) // page, 1.0, 0.0
    ).astype(bf16)
    found = dot(table, spread)
    code = found[:SIDE]
    for b in range(1, BLOCK):
        code = code + found[b * SIDE : (b + 1) * SIDE]
    code = code.astype(jnp.int32) - 1
    key_ref[...] = jnp.where(iota(code.shape, 1) % page <= (code & (page - 1)), code >> 4, -1)

    q = q_ref[...]
    scale = math.log2(math.e) / math.sqrt(dim)
    wanted = iota((requests, span), 0)
    highest = jnp.full((rows, 128), lowest, f32)
    for c in range(steps):
        copies[c][0].wait()
        for i in range(c * CHUNK // span, (c + 1) * CHUNK // span):
            here = slice(i * span, (i + 1) * span)
            bias = jnp.where(key_ref[i : i + 1, :] == wanted, 0.0, masked)
            s = dot_t(q, k_buf[here, :]) * scale + jnp.concatenate([bias] * heads, axis=0)
            s_buf[:, here] = s
            for j in range(span // 128):
                highest = jnp.maximum(highest, s[:, j * 128 : (j + 1) * 128])
    top = jnp.max(highest, axis=1, keepdims=True)
    total = jnp.zeros((rows, 128), f32)
    out = jnp.zeros((rows, dim), f32)
    for c in range(steps):
        copies[c][1].wait()
        for i in range(c * CHUNK // STRIDE, (c + 1) * CHUNK // STRIDE):
            here = slice(i * STRIDE, (i + 1) * STRIDE)
            p = jnp.exp2(s_buf[:, here] - top)
            for j in range(STRIDE // 128):
                total = total + p[:, j * 128 : (j + 1) * 128]
            out = out + dot(p.astype(bf16), v_buf[here, :])
    total = jnp.sum(total, axis=1, keepdims=True)

    nk = jnp.concatenate([nk_ref[...].astype(f32)] * heads, axis=0)
    nv = jnp.concatenate([nv_ref[...].astype(f32)] * heads, axis=0)
    self_score = jnp.sum(q.astype(f32) * nk, axis=1, keepdims=True)
    self_score = jnp.where(me == 0, self_score * scale, masked)
    new_top = jnp.maximum(top, self_score)
    keep = jnp.exp2(top - new_top)
    take = jnp.exp2(self_score - new_top)
    out = out * keep + take * nv
    total = total * keep + take

    meta = jnp.zeros((rows, 128), f32)
    for i, part in enumerate(split3(new_top) + split3(total)):
        meta = jnp.where(lane == 6 * group + i, part, meta)
    both = jnp.concatenate([out.astype(bf16), meta.astype(bf16)], axis=0)
    out_ref[...] = dot(pick, both).astype(bf16)


def near_kernel(got_ref, out_ref):
    sent = got_ref.shape[0]
    blocks = sent // (4 * NEAR)
    mine = 3 * blocks
    kept = mine + 8
    got = got_ref[...]
    height = 2 * NEAR * kept
    to = iota((height, sent), 0)
    source = iota((height, sent), 1)
    line = to % kept
    near = (to // kept) % NEAR
    base = (line // 3) * (4 * NEAR) + near * 4
    wanted = jnp.where(to < NEAR * kept, base + line % 3, base + 3)
    pick = jnp.where((source == wanted) & (line < mine), 1.0, 0.0).astype(bf16)
    all_rows = dot(pick, got)
    lane = iota((kept, 128), 1)
    line = iota((kept, 128), 0)
    first = 6 * (line % 3)
    outs, tops, totals = [], [], []
    for b in range(NEAR):
        outs.append(all_rows[b * kept : (b + 1) * kept])
        meta = all_rows[(NEAR + b) * kept : (NEAR + b + 1) * kept]
        is_top = (lane >= first) & (lane < first + 3)
        is_total = (lane >= first + 3) & (lane < first + 6)
        tops.append(jnp.sum(jnp.where(is_top, meta, 0.0), axis=1, keepdims=True))
        totals.append(jnp.sum(jnp.where(is_total, meta, 0.0), axis=1, keepdims=True))
    top = tops[0]
    for t in tops[1:]:
        top = jnp.maximum(top, t)
    out = jnp.zeros((kept, 128), f32)
    total = jnp.zeros((kept, 1), f32)
    for b in range(NEAR):
        factor = jnp.exp2(tops[b] - top)
        out = out + factor * outs[b]
        total = total + factor * totals[b]
    meta = jnp.zeros((kept, 128), f32)
    for i, part in enumerate(split3(top) + split3(total)[:2]):
        meta = jnp.where((lane == line + i * mine) & (line < mine), part, meta)
    out = jnp.where(line == mine, jnp.sum(meta, axis=0, keepdims=True), out)
    block = mine + 2
    out = out.astype(bf16)[:block]
    for d in range(out_ref.shape[0] // block):
        out_ref[d * block : (d + 1) * block, :] = out


def project_kernel(got_ref, w_ref, out_ref, flat_ref, *, block):
    total_rows, dim = got_ref.shape
    far = total_rows // block // NEAR
    mine = block - 2
    flat_ref[...] = jnp.zeros(flat_ref.shape, f32)
    lane = iota((mine, 128), 1)
    line = iota((mine, 128), 0)
    is_top = (lane % mine == line) & (lane < 3 * mine)
    is_total = (lane % mine == line) & (lane >= 3 * mine) & (lane < 5 * mine)
    for b in range(NEAR):
        outs, tops, totals = [], [], []
        for a in range(far):
            first = (a * NEAR + b) * block
            x = got_ref[first : first + block, :].astype(f32)
            head = x[mine : mine + 1]
            outs.append(x[:mine])
            tops.append(jnp.sum(jnp.where(is_top, head, 0.0), axis=1, keepdims=True))
            totals.append(jnp.sum(jnp.where(is_total, head, 0.0), axis=1, keepdims=True))
        top = tops[0]
        for t in tops[1:]:
            top = jnp.maximum(top, t)
        out = jnp.zeros((mine, dim), f32)
        total = jnp.zeros((mine, 1), f32)
        for a in range(far):
            factor = jnp.exp2(tops[a] - top)
            out = out + factor * outs[a]
            total = total + factor * totals[a]
        attended = out / total
        halves = NEAR // 2
        request, half = b // halves, b % halves
        for i in range(mine):
            at = ((i // 3) * 3 * halves + half * 3 + i % 3) * dim
            flat_ref[request : request + 1, at : at + dim] = attended[i : i + 1]
    projected = dot(flat_ref[...].astype(bf16), w_ref[...])
    out_ref[...] = projected[: out_ref.shape[0]].astype(bf16)


VMEM = pl.BlockSpec(memory_space=pltpu.VMEM)
ANY = pl.BlockSpec(memory_space=pl.ANY)


def local(
    queries, k_cache, v_cache, new_key, new_value, ctx_lens, page_owner, page_slot, out_weight,
    interpret=False,
):
    _, slots, page, dim = k_cache.shape
    requests, heads, _ = queries.shape
    tokens = slots * page
    rows = requests * heads
    sent = rows // 3 * 4
    partial = attend_call(
        lambda: lax.axis_index(("far", "near")), ctx_lens, page_owner, page_slot, queries.transpose(1, 0, 2).reshape(rows, dim), new_key[0], new_value[0],
        k_cache.reshape(tokens, dim), v_cache.reshape(tokens, dim), sent, interpret,
    )
    partial, out_weight = lax.optimization_barrier((partial, out_weight))
    got = lax.all_to_all(partial, ("heads", "near"), 0, 0, tiled=True)
    peers = lax.axis_size("far") * lax.axis_size("near")
    merged = near_call(got, peers, interpret)
    block = merged.shape[0] // peers
    merged = merged.reshape(peers, block // 2, 2, dim)
    everything = lax.all_to_all(merged, ("far", "near"), 0, 0, tiled=True)
    everything = everything.reshape(peers * block, dim)
    mine = requests // lax.axis_size("heads")
    return project_call(everything, out_weight, mine, block, interpret)


def in_hbm(x):
    return pltpu.with_memory_space_constraint(x, pltpu.HBM)


def attend_call(position, lens, owner, slot, q, nk, nv, k, v, sent, interpret):
    tokens, dim = k.shape
    requests, max_pages = owner.shape
    return pl.pallas_call(
        lambda *refs: attend_kernel(*refs, position=position),
        out_shape=jax.ShapeDtypeStruct((sent, dim), bf16),
        in_specs=[ANY] * 8,
        out_specs=VMEM,
        scratch_shapes=[
            pltpu.SMEM(lens.shape, lens.dtype),
            *(pltpu.VMEM(x.shape, x.dtype) for x in (owner, slot, q, nk, nv)),
            pltpu.VMEM((tokens, dim), bf16),
            pltpu.VMEM((tokens, dim), bf16),
            pltpu.VMEM((q.shape[0], tokens), f32),
            pltpu.VMEM((requests, max_pages), jnp.int32),
            pltpu.VMEM((requests, max_pages), jnp.int32),
            pltpu.VMEM((requests, max_pages), f32),
            pltpu.VMEM((SIDE, tokens // SIDE), jnp.int32),
            pltpu.SemaphoreType.DMA((6,)),
            pltpu.SemaphoreType.DMA((2, tokens // CHUNK)),
        ],
        compiler_params=pltpu.CompilerParams(vmem_limit_bytes=24 << 20),
        interpret=interpret,
        name="attend",
    )(*(in_hbm(x) for x in (lens, owner, slot, q, nk, nv, k, v)))


def near_call(got, peers, interpret):
    sent, dim = got.shape
    block = sent // (4 * NEAR) * 3 + 2
    return pl.pallas_call(
        near_kernel,
        out_shape=jax.ShapeDtypeStruct((peers * block, dim), bf16),
        in_specs=[VMEM],
        out_specs=VMEM,
        compiler_params=pltpu.CompilerParams(vmem_limit_bytes=4 << 20),
        interpret=interpret,
        name="near",
    )(got)


def project_call(everything, w, mine, block, interpret):
    inner, features = w.shape
    return pl.pallas_call(
        lambda *refs: project_kernel(*refs, block=block),
        out_shape=jax.ShapeDtypeStruct((mine, features), bf16),
        in_specs=[VMEM, VMEM],
        out_specs=VMEM,
        scratch_shapes=[pltpu.VMEM((8, inner), f32)],
        compiler_params=pltpu.CompilerParams(vmem_limit_bytes=8 << 20),
        interpret=interpret,
        name="project",
    )(everything, pltpu.with_memory_space_constraint(w, pltpu.VMEM))


def solution(mesh):
    torus = Mesh(
        mesh.devices.reshape(
            mesh.shape["group"], mesh.shape["pages"] // NEAR, NEAR, mesh.shape["heads"]
        ),
        ("group", "far", "near", "heads"),
    )
    pages = ("far", "near")
    in_specs = (
        P("group", "heads", None),
        P("heads", ("group", *pages), None, None),
        P("heads", ("group", *pages), None, None),
        P("heads", "group", None),
        P("heads", "group", None),
        P("group"),
        P("group", None),
        P("group", None),
        P(None, pages),
    )
    out_specs = P(("group", "heads"), pages)
    return jax.shard_map(local, mesh=torus, in_specs=in_specs, out_specs=out_specs, check_vma=False)
```
